128 devices in a mesh: dom: 32 (over z, y, core), sub: 4 (over x).
Axes of the slice: x: 4, y: 4, z: 4, core: 2. Of those that a mesh axis runs over, the one named last changes fastest.
Arguments:
- node_state: bfloat16 [64, 131072], P(None, ('dom', 'sub')), may hold values from -6 to 6
- edge_state: bfloat16 [64, 393216], P(None, ('dom', 'sub')), may hold values from -6 to 6
- senders: int32 [393216], P(('dom', 'sub')), may hold values from 0 to 2559, as said below
- receivers: int32 [393216], P(('dom', 'sub')), may hold values from 0 to 1023
- send_index: int32 [128, 12, 128], P(('dom', 'sub')), may hold values from -1 to 1023, as said below
- node_cotangent: bfloat16 [64, 131072], P(None, ('dom', 'sub')), may hold values from -6 to 6
- edge_cotangent: bfloat16 [64, 393216], P(None, ('dom', 'sub')), may hold values from -6 to 6
- edge_first: bfloat16 [192, 64], replicated, may hold values from -0.4375 to 0.4375
- edge_bias: float32 [64], replicated, may hold values from -3 to 3
- edge_second: bfloat16 [64, 64], replicated, may hold values from -0.75 to 0.75
- edge_gain: float32 [64], replicated, may hold values from 0.1 to 1.9
- edge_shift: float32 [64], replicated, may hold values from -3 to 3
- node_first: bfloat16 [128, 64], replicated, may hold values from -0.5 to 0.5
- node_bias: float32 [64], replicated, may hold values from -3 to 3
- node_second: bfloat16 [64, 64], replicated, may hold values from -0.75 to 0.75
- node_gain: float32 [64], replicated, may hold values from 0.1 to 1.9
Outputs:
- delta_state: bfloat16 [64, 131072], P(None, ('dom', 'sub'))
- delta_edges: bfloat16 [64, 393216], P(None, ('dom', 'sub'))
- delta_edgefirst: float32 [192, 64], replicated
- delta_edgebias: float32 [64], replicated
- delta_edgesecond: float32 [64, 64], replicated
- delta_edgegain: float32 [64], replicated
- delta_edgeshift: float32 [64], replicated
- delta_nodefirst: float32 [128, 64], replicated
- delta_nodebias: float32 [64], replicated
- delta_nodesecond: float32 [64, 64], replicated
- delta_nodegain: float32 [64], replicated
- delta_nodeshift: float32 [64], replicated
The draws below stay inside these ranges and needn't reach their ends.
Inputs may be any that keep to these rules, and one draw needn't show every extreme that they name: `send_index`: block k = o * 4 + t of partition p = d * 4 + s lists own cells that p sends to the partition at dom index d + o - 1 and sub index t: live entries first, then -1. Blocks towards a dom index outside the mesh, and block 4 + s, hold only -1; every other block holds 32 to 128 live entries. Some partition receives a full block from every partition that sends to it. `senders`: an entry below 1024 is an own cell. An entry 1024 + k * 128 + j with k = o * 4 + u names ghost slot j of block k: the j-th entry of block o * 4 + s of the partition at dom index d + 1 - o and sub index u, and that entry is live.
All inputs are finite; a program needn't handle non-finite values.
Results may differ from the reference program's by a relative error of at most 0.0095.
Values may be sent and summed in bfloat16 or wider, within the bound.
A program may use at most 64 MiB of HBM per device.

```python
import math
import jax
import jax.numpy as jnp
from jax import lax

D = 64
HIDDEN_SIZE = 64
CELLS_DEV = 1024
HALO = 128
FACES_DEV = 3072
PARTITIONS = 128
PEERS = 12
GHOST = 1536
CELLS = 131072
FACES = 393216
N_DOM = 32
N_SUB = 4


def halo_counts(key):
    base_key = jax.random.fold_in(key, 7)
    count_key, target_key = jax.random.split(base_key)
    live_count = jax.random.randint(count_key, (PARTITIONS, PEERS), HALO // 4, HALO + 1)
    partition = jnp.arange(PARTITIONS, dtype=jnp.int32)[:, None]
    peer_slot = jnp.arange(PEERS, dtype=jnp.int32)[None, :]
    target_row = partition // N_SUB + peer_slot // N_SUB - 1
    sub_here = partition % N_SUB
    exists = (target_row >= 0) & (target_row < N_DOM) & jnp.logical_not((peer_slot // N_SUB == 1) & (peer_slot % N_SUB == sub_here))
    chosen = jax.random.randint(target_key, (), N_SUB, PARTITIONS)
    target = target_row * N_SUB + peer_slot % N_SUB
    receives_full = target == chosen
    counts = jnp.where(receives_full, HALO, live_count)
    return jnp.where(exists, counts, 0).astype(jnp.int32)


def draw_send_index(key, part):
    counts = halo_counts(key)
    cell_draw = jax.random.randint(jax.random.fold_in(key, 11), (PARTITIONS, PEERS, HALO), 0, CELLS_DEV)
    slot_position = jnp.arange(HALO, dtype=jnp.int32)[None, None, :]
    return jnp.where(slot_position < counts[:, :, None], cell_draw, -1).astype(jnp.int32)


def draw_senders(key, part):
    counts = halo_counts(key)
    partition = jnp.arange(PARTITIONS, dtype=jnp.int32)[:, None]
    peer_slot = jnp.arange(PEERS, dtype=jnp.int32)[None, :]
    source_row = partition // N_SUB + 1 - peer_slot // N_SUB
    source_ok = (source_row >= 0) & (source_row < N_DOM)
    source = jnp.clip(source_row * N_SUB + peer_slot % N_SUB, 0, PARTITIONS - 1)
    mirror_slot = peer_slot // N_SUB * N_SUB + partition % N_SUB
    incoming = jnp.where(source_ok, counts[source, mirror_slot], 0)
    key_list = jax.random.split(jax.random.fold_in(key, 23), 4)
    local_cells = jax.random.randint(key_list[0], (PARTITIONS, FACES_DEV), 0, CELLS_DEV)
    chosen_peer = jax.random.randint(key_list[1], (PARTITIONS, FACES_DEV), 0, PEERS)
    position = jax.random.randint(key_list[2], (PARTITIONS, FACES_DEV), 0, HALO)
    want_ghost = jax.random.randint(key_list[3], (PARTITIONS, FACES_DEV), 0, 8) == 0
    face_number = jnp.arange(FACES_DEV, dtype=jnp.int32)[None, :]
    last_face = face_number == FACES_DEV - 1
    chosen_peer = jnp.where(last_face, PEERS - 1, chosen_peer)
    available = jnp.take_along_axis(incoming, chosen_peer, axis=1)
    position = jnp.where(last_face, available - 1, position % jnp.maximum(available, 1))
    use_ghost = (want_ghost | last_face) & (available > 0)
    ghost_index = CELLS_DEV + chosen_peer * HALO + position
    return jnp.where(use_ghost, ghost_index, local_cells).reshape(-1).astype(jnp.int32)


def place_ends(values, own_key, low, largest):
    shape = values.shape
    spot = [jax.random.randint(jax.random.fold_in(own_key, axis), (), 0, shape[axis]) for axis in range(len(shape))]
    values = values.at[tuple(spot)].set(low)
    longest = shape.index(max(shape))
    spot[longest] = (spot[longest] + 1) % shape[longest]
    return values.at[tuple(spot)].set(largest)


def level_of(key, extent, cuts, low, largest):
    level, own = 1.0, jax.random.fold_in(key, 6)
    for axis_at, shards_of in cuts:
        heights = jnp.exp(jax.random.uniform(jax.random.fold_in(own, axis_at), (shards_of,), jnp.float32, low / len(cuts), largest / len(cuts)))
        level = level * jnp.repeat(heights, extent[axis_at] // shards_of).reshape([-1 if axis == axis_at else 1 for axis in range(len(extent))])
    return level


def scatter_about(rng, shape, deviation, most, cuts=(), kind=jnp.bfloat16):
    factor_of = level_of(rng, shape, cuts, -0.22, 0.18) if cuts else 1.0
    values = jax.random.normal(rng, shape, jnp.float32) * deviation * factor_of
    return jnp.minimum(jnp.maximum(values, -most), most).astype(kind)


def setup_inputs(seed: int = 0) -> dict:
    splits = jax.random.split(jax.random.key(seed), 17)
    return {
        "node_state": scatter_about(splits[0], (D, CELLS), 1.0, 6.0, ((1, 128),)),
        "edge_state": scatter_about(splits[1], (D, FACES), 1.0, 6.0, ((1, 128),)),
        "senders": draw_senders(jax.random.fold_in(splits[16], 71), 0),
        "receivers": place_ends(jax.random.randint(splits[3], (FACES,), 0, CELLS_DEV), jax.random.fold_in(splits[3], 1), 0, CELLS_DEV - 1).astype(jnp.int32),
        "send_index": draw_send_index(jax.random.fold_in(splits[16], 71), 0),
        "node_cotangent": scatter_about(splits[5], (D, CELLS), 1.0, 6.0, ((1, 128),)),
        "edge_cotangent": scatter_about(splits[6], (D, FACES), 1.0, 6.0, ((1, 128),)),
        "edge_first": scatter_about(splits[7], (3 * D, HIDDEN_SIZE), (3 * D) ** -0.5, 0.4375),
        "edge_bias": scatter_about(splits[8], (HIDDEN_SIZE,), 0.5, 3.0, (), jnp.float32),
        "edge_second": scatter_about(splits[9], (HIDDEN_SIZE, D), HIDDEN_SIZE ** -0.5, 0.75),
        "edge_gain": jnp.clip(1.0 + 0.18 * jax.random.normal(splits[10], (D,), jnp.float32), 0.1, 1.9),
        "edge_shift": scatter_about(splits[11], (D,), 0.5, 3.0, (), jnp.float32),
        "node_first": scatter_about(splits[12], (2 * D, HIDDEN_SIZE), (2 * D) ** -0.5, 0.5),
        "node_bias": scatter_about(splits[13], (HIDDEN_SIZE,), 0.5, 3.0, (), jnp.float32),
        "node_second": scatter_about(splits[14], (HIDDEN_SIZE, D), HIDDEN_SIZE ** -0.5, 0.75),
        "node_gain": jnp.clip(1.0 + 0.18 * jax.random.normal(splits[15], (D,), jnp.float32), 0.1, 1.9),
    }


EPSILON = 1e-05

def contract_first(first_operand, second_operand):
    return lax.dot_general(first_operand, second_operand, (((0,), (0,)), ((), ())), preferred_element_type=jnp.float32)

def contract_last(first_operand, second_operand):
    return lax.dot_general(first_operand, second_operand, (((1,), (1,)), ((), ())), preferred_element_type=jnp.float32)

def sigmoid_linear(values):
    return values * jax.nn.sigmoid(values)

def sigmoid_slope(values):
    logistic = jax.nn.sigmoid(values)
    return logistic * (1.0 + values * (1.0 - logistic))

def standardize(values):
    centered = values - lax.optimization_barrier(jnp.mean(values, axis=0, keepdims=True))
    spread = lax.rsqrt(lax.optimization_barrier(jnp.mean(centered * centered, axis=0, keepdims=True)) + EPSILON)
    return (centered * spread, spread)

def normalize_back(upstream, scaled, spread, gain_vector):
    gain_delta = lax.optimization_barrier(jnp.sum(upstream * scaled, axis=1))
    shift_delta = lax.optimization_barrier(jnp.sum(upstream, axis=1))
    weighted = upstream * gain_vector[:, None]
    result = spread * (weighted - lax.optimization_barrier(jnp.mean(weighted, axis=0, keepdims=True)) - scaled * lax.optimization_barrier(jnp.mean(weighted * scaled, axis=0, keepdims=True)))
    return (result, gain_delta, shift_delta)

def local_backward(extended, node_state, edge_state, senders, receivers, node_cotangent, edge_cotangent, edge_first, edge_bias, edge_second, edge_gain, edge_shift, node_first, node_bias, node_second, node_gain):
    features, cell_count = node_state.shape
    sender_rows = jnp.take(extended, senders, axis=1)
    receiver_rows = jnp.take(node_state, receivers, axis=1)
    stacked = jnp.concatenate([sender_rows, receiver_rows, edge_state], axis=0)
    edge_linear = contract_first(edge_first, stacked) + edge_bias[:, None]
    edge_active = sigmoid_linear(edge_linear).astype(jnp.bfloat16)
    edge_output = contract_first(edge_second, edge_active)
    edge_scaled, edge_spread = standardize(edge_output)
    message = (edge_scaled * edge_gain[:, None] + edge_shift[:, None]).astype(jnp.bfloat16)
    summed = jnp.zeros((features, cell_count), jnp.float32).at[:, receivers].add(message.astype(jnp.float32))
    node_input = jnp.concatenate([node_state, summed.astype(jnp.bfloat16)], axis=0)
    node_linear = contract_first(node_first, node_input) + node_bias[:, None]
    node_active = sigmoid_linear(node_linear).astype(jnp.bfloat16)
    node_output = contract_first(node_second, node_active)
    node_scaled, node_spread = standardize(node_output)
    upstream = node_cotangent.astype(jnp.float32)
    node_delta, nodegain_delta, nodeshift_delta = normalize_back(upstream, node_scaled, node_spread, node_gain)
    node_delta = node_delta.astype(jnp.bfloat16)
    nodesecond_delta = contract_last(node_active, node_delta)
    node_hidden = jnp.dot(node_second, node_delta, preferred_element_type=jnp.float32) * sigmoid_slope(node_linear)
    nodebias_delta = lax.optimization_barrier(jnp.sum(node_hidden, axis=1))
    node_hidden = node_hidden.astype(jnp.bfloat16)
    nodefirst_delta = contract_last(node_input, node_hidden)
    node_back = jnp.dot(node_first, node_hidden, preferred_element_type=jnp.float32)
    message_delta = edge_cotangent.astype(jnp.float32) + jnp.take(node_back[features:], receivers, axis=1)
    edge_delta, edgegain_delta, edgeshift_delta = normalize_back(message_delta, edge_scaled, edge_spread, edge_gain)
    edge_delta = edge_delta.astype(jnp.bfloat16)
    edgesecond_delta = contract_last(edge_active, edge_delta)
    edge_hidden = jnp.dot(edge_second, edge_delta, preferred_element_type=jnp.float32) * sigmoid_slope(edge_linear)
    edgebias_delta = lax.optimization_barrier(jnp.sum(edge_hidden, axis=1))
    edge_hidden = edge_hidden.astype(jnp.bfloat16)
    edgefirst_delta = contract_last(stacked, edge_hidden)
    edge_back = jnp.dot(edge_first, edge_hidden, preferred_element_type=jnp.float32)
    edge_result = (edge_cotangent.astype(jnp.float32) + edge_back[2 * features:]).astype(jnp.bfloat16)
    scattered = jnp.zeros(extended.shape, jnp.float32).at[:, senders].add(edge_back[:features])
    local_delta = scattered[:, :cell_count].at[:, receivers].add(edge_back[features:2 * features]) + node_back[:features] + upstream
    ghost_delta = scattered[:, cell_count:]
    partials = (edgefirst_delta, edgebias_delta, edgesecond_delta, edgegain_delta, edgeshift_delta, nodefirst_delta, nodebias_delta, nodesecond_delta, nodegain_delta, nodeshift_delta)
    return (local_delta, ghost_delta, edge_result, partials)

def reference(node_state, edge_state, senders, receivers, send_index, node_cotangent, edge_cotangent, edge_first, edge_bias, edge_second, edge_gain, edge_shift, node_first, node_bias, node_second, node_gain):
    features = node_state.shape[0]
    partition = jnp.arange(PARTITIONS, dtype=jnp.int32)[:, None]
    peer_slot = jnp.arange(PEERS, dtype=jnp.int32)[None, :]
    slot_position = jnp.arange(HALO, dtype=jnp.int32)[None, None, :]
    mirror_slot = peer_slot // N_SUB * N_SUB + partition % N_SUB
    source_row = partition // N_SUB + 1 - peer_slot // N_SUB
    source_ok = (source_row >= 0) & (source_row < N_DOM)
    source = jnp.clip(source_row * N_SUB + peer_slot % N_SUB, 0, PARTITIONS - 1)
    incoming = send_index[source, mirror_slot]
    live_in = source_ok[:, :, None] & (incoming >= 0)
    global_in = source[:, :, None] * CELLS_DEV + jnp.maximum(incoming, 0)
    gathered = jnp.take(node_state, global_in.reshape(-1).astype(jnp.int32), axis=1)
    ghost_cells = jnp.where(live_in.reshape(1, -1), gathered, jnp.zeros_like(gathered))
    weight_shapes = (edge_first.shape, edge_bias.shape, edge_second.shape, edge_gain.shape, edge_gain.shape, node_first.shape, node_bias.shape, node_second.shape, node_gain.shape, node_gain.shape)
    initial = (jnp.zeros((features, CELLS), jnp.float32), jnp.zeros((features, PARTITIONS * GHOST), jnp.float32), jnp.zeros((features, FACES), jnp.bfloat16), tuple((jnp.zeros(shape, jnp.float32) for shape in weight_shapes)))

    def one_partition(loop_index, carried):
        local_all, ghost_all, edge_all, weight_all = carried
        cell_start = (loop_index * CELLS_DEV).astype(jnp.int32)
        face_start = (loop_index * FACES_DEV).astype(jnp.int32)
        ghost_start = (loop_index * GHOST).astype(jnp.int32)
        state_block = lax.dynamic_slice_in_dim(node_state, cell_start, CELLS_DEV, 1)
        ghost_block = lax.dynamic_slice_in_dim(ghost_cells, ghost_start, GHOST, 1)
        extended = jnp.concatenate([state_block, ghost_block], axis=1)
        outcome = local_backward(extended, state_block, lax.dynamic_slice_in_dim(edge_state, face_start, FACES_DEV, 1), lax.dynamic_slice_in_dim(senders, face_start, FACES_DEV, 0), lax.dynamic_slice_in_dim(receivers, face_start, FACES_DEV, 0), lax.dynamic_slice_in_dim(node_cotangent, cell_start, CELLS_DEV, 1), lax.dynamic_slice_in_dim(edge_cotangent, face_start, FACES_DEV, 1), edge_first, edge_bias, edge_second, edge_gain, edge_shift, node_first, node_bias, node_second, node_gain)
        local_delta, ghost_delta, edge_result, partials = outcome
        local_all = lax.dynamic_update_slice_in_dim(local_all, local_delta, cell_start, 1)
        ghost_all = lax.dynamic_update_slice_in_dim(ghost_all, ghost_delta, ghost_start, 1)
        edge_all = lax.dynamic_update_slice_in_dim(edge_all, edge_result, face_start, 1)
        weight_all = tuple((running + portion for running, portion in zip(weight_all, partials)))
        return (local_all, ghost_all, edge_all, weight_all)
    local_all, ghost_all, edge_all, weight_all = lax.fori_loop(0, PARTITIONS, one_partition, initial)
    target_row = partition // N_SUB + peer_slot // N_SUB - 1
    target_ok = (target_row >= 0) & (target_row < N_DOM)
    target = jnp.clip(target_row * N_SUB + peer_slot % N_SUB, 0, PARTITIONS - 1)
    live_out = target_ok[:, :, None] & (send_index >= 0)
    from_index = (target * PEERS + mirror_slot)[:, :, None] * HALO + slot_position
    coming_back = jnp.take(ghost_all, from_index.reshape(-1).astype(jnp.int32), axis=1)
    coming_back = jnp.where(live_out.reshape(1, -1), coming_back, jnp.zeros_like(coming_back))
    to_index = partition[:, :, None] * CELLS_DEV + jnp.maximum(send_index, 0)
    local_all = local_all.at[:, to_index.reshape(-1).astype(jnp.int32)].add(coming_back)
    factor = 1.0 / math.sqrt(FACES)
    edgefirst_sum, edgebias_sum, edgesecond_sum, edgegain_sum, edgeshift_sum, nodefirst_sum, nodebias_sum, nodesecond_sum, nodegain_sum, nodeshift_sum = weight_all
    return (local_all.astype(jnp.bfloat16), edge_all, edgefirst_sum * factor, edgebias_sum * factor, edgesecond_sum * factor, edgegain_sum * factor, edgeshift_sum * factor, nodefirst_sum * factor, nodebias_sum * factor, nodesecond_sum * factor, nodegain_sum * factor, nodeshift_sum * factor)
```

```python
import math

import jax
import jax.numpy as jnp
from jax import lax
from jax.experimental import pallas as pl
from jax.experimental.pallas import tpu as pltpu
from jax.sharding import Mesh
from jax.sharding import PartitionSpec as P

AXES = ("z", "y", "core", "sub")
MESH = pl.DeviceIdType.MESH
EPSILON = 1e-05
D = 64
NF = 3072
NC = 1024
NB = 12
HALO = 128
BLK = 512
bf16 = jnp.bfloat16
f32 = jnp.float32
FACTOR = 1.0 / math.sqrt(393216)


def mm(a, b):
    return jnp.dot(a, b, preferred_element_type=f32)


def mm_last(a, b):
    return lax.dot_general(a, b, (((1,), (1,)), ((), ())), preferred_element_type=f32)


def split_index(row):
    return row & 255, row >> 8


def sub_iota(width):
    return lax.broadcasted_iota(jnp.int32, (256, width), 0).astype(f32).astype(bf16)


def selector(lo, hi, tile, iota):
    key = jnp.where(hi == tile, lo, -1).astype(f32).astype(bf16)
    return jnp.where(iota == key, bf16(1), bf16(0))


def columns_of(lo, hi):
    width = lo.shape[1]
    row = lax.broadcasted_iota(jnp.int32, (8, width), 0)
    stacked = jnp.where(row == 0, lo, jnp.where(row == 1, hi, 0)).astype(f32)
    sub = lax.broadcasted_iota(jnp.int32, (8, 256), 0)
    lane = lax.broadcasted_iota(jnp.int32, (8, 256), 1)
    chooser = jnp.where(((sub == 0) & (lane < 128)) | ((sub == 1) & (lane >= 128)), 1.0, 0.0)
    out = lax.dot_general(
        stacked, chooser, (((0,), (0,)), ((), ())), preferred_element_type=f32
    )
    return out.astype(bf16)


def lane_iotas():
    lane = lax.broadcasted_iota(jnp.int32, (1, 128), 1)
    return lane.astype(f32).astype(bf16), (lane + 128).astype(f32).astype(bf16)


def selector_t(lo, hi, tile, iotas):
    key = jnp.where(hi == bf16(tile), lo, bf16(-1))
    return jnp.concatenate(
        [jnp.where(key == lanes, bf16(1), bf16(0)) for lanes in iotas], axis=1
    )


def column_of(row):
    sub = lax.broadcasted_iota(jnp.int32, (D, D), 0)
    lane = lax.broadcasted_iota(jnp.int32, (D, D), 1)
    col = jnp.sum(jnp.where(sub == lane, row, 0.0), axis=1, keepdims=True)
    return jnp.broadcast_to(col, (D, 128))


def wide(col, width):
    return jnp.concatenate([col] * (width // 128), axis=1)


def fold_lanes(values):
    total = values[:, 0:128]
    for begin in range(128, values.shape[1], 128):
        total = total + values[:, begin : begin + 128]
    return total


def mean_rows(values):
    return jnp.sum(values, axis=0, keepdims=True) * (1.0 / D)


def logistic(values):
    return 0.5 * jnp.tanh(0.5 * values) + 0.5


def standardize(values):
    centered = values - mean_rows(values)
    spread = lax.rsqrt(mean_rows(centered * centered) + EPSILON)
    return centered * spread, spread


def normalize_back(upstream, scaled, spread, gain):
    weighted = upstream * gain
    return spread * (weighted - mean_rows(weighted) - scaled * mean_rows(weighted * scaled))


def make_kernel(comm):
    def kernel(
        ns, es, snd, rcv, six, nct, ect, w1, b1, w2, eg, esh, nw1, nb1, nw2, ng,
        dstate, dedges, o_w1, o_b1, o_w2, o_eg, o_es, o_nw1, o_nb1, o_nw2, o_ng, o_ns,
        stk, slope, scl, spr, msg, ehd, col_s, col_r, col_p,
        sendb, ghost, gsend, gback, nin, nh2, nbr, own, acc, gt, gsb,
        vec, sums, grads, rs_buf, ex_buf, ag_buf, w1t, w2t, nw1t, nw2t,
        sem_fs, sem_fr, sem_bs, sem_br, sem_rs, sem_rr, sem_es, sem_er, sem_as, sem_ar,
    ):
        if comm:
            z = lax.axis_index("z")
            y = lax.axis_index("y")
            core = lax.axis_index("core")
            s = lax.axis_index("sub")
            d = z * 8 + y * 2 + core
            a = z * 2 + core
            b = y * 4 + s

            def row_peer(step, r):
                dd = lax.rem(d + (step + 32), 32)
                return (
                    lax.div(dd, 8),
                    lax.rem(lax.div(dd, 2), 4),
                    lax.rem(dd, 2),
                    lax.rem(s + r, 4),
                )

            def a_peer(j):
                other = lax.rem(a + j, 8)
                return other, (lax.div(other, 2), y, lax.rem(other, 2), s)

            def b_peer(j):
                other = lax.rem(b + j, 16)
                return other, (z, lax.div(other, 4), core, lax.rem(other, 4))

            halo_pairs = [(o, r) for o in range(3) for r in range(4) if not (o == 1 and r == 0)]
            barrier = pltpu.get_barrier_semaphore()
            peers = [row_peer(o - 1, r) for o, r in halo_pairs]
            peers += [a_peer(j)[1] for j in range(1, 8)] + [b_peer(j)[1] for j in range(1, 16)]
            for peer in peers:
                pl.semaphore_signal(barrier, inc=1, device_id=peer, device_id_type=MESH)
        else:
            s = 0

        iota = sub_iota(256)
        iota2 = jnp.concatenate([iota, iota], axis=1)
        iotas = lane_iotas()

        for pair in range(NB // 2):
            row = jnp.concatenate([six[2 * pair : 2 * pair + 1, :], six[2 * pair + 1 : 2 * pair + 2, :]], axis=1)
            lo, hi = split_index(row)
            picked = jnp.zeros((D, 256), f32)
            for tile in range(4):
                picked = picked + mm(
                    ns[:, 256 * tile : 256 * tile + 256], selector(lo, hi, tile, iota)
                )
            picked = picked.astype(bf16)
            sendb[2 * pair] = picked[:, :HALO]
            sendb[2 * pair + 1] = picked[:, HALO:]
            col_p[256 * pair : 256 * pair + 256, :] = columns_of(lo, hi)

        ghost[4 + s] = jnp.zeros((D, HALO), bf16)
        gback[4 + s] = jnp.zeros((D, HALO), bf16)

        forward = []
        backward = []
        if comm:
            pl.semaphore_wait(barrier, len(peers))
            for number, (o, r) in enumerate(halo_pairs):
                t = lax.rem(s + r, 4)
                forward.append(
                    pltpu.make_async_remote_copy(
                        src_ref=sendb.at[o * 4 + t],
                        dst_ref=ghost.at[o * 4 + s],
                        send_sem=sem_fs.at[number],
                        recv_sem=sem_fr.at[o * 4 + s],
                        device_id=row_peer(o - 1, r),
                        device_id_type=MESH,
                    )
                )
            for copy in forward:
                copy.start()

        vec[0] = column_of(b1[...])
        vec[1] = column_of(eg[...])
        vec[2] = column_of(esh[...])
        vec[3] = column_of(nb1[...])
        vec[4] = column_of(ng[...])
        w1t[...] = w1[...].astype(f32).T.astype(bf16)
        w2t[...] = w2[...].astype(f32).T.astype(bf16)
        nw1t[...] = nw1[...].astype(f32).T.astype(bf16)
        nw2t[...] = nw2[...].astype(f32).T.astype(bf16)
        sums[...] = jnp.zeros_like(sums)
        stk[128:192, :] = es[...]
        nin[0:64, :] = ns[...]

        def gather_own(i, carry):
            at = pl.ds(pl.multiple_of(i * BLK, BLK), BLK)
            for index, begin, cols in ((snd, 0, col_s), (rcv, 64, col_r)):
                lo, hi = split_index(index[:, at])
                total = jnp.zeros((D, BLK), f32)
                for tile in range(4):
                    total = total + mm(
                        ns[:, 256 * tile : 256 * tile + 256], selector(lo, hi, tile, iota2)
                    )
                stk[begin : begin + 64, at] = total.astype(bf16)
                cols[at, :] = columns_of(lo, hi)
            return carry

        lax.fori_loop(0, NF // BLK, gather_own, 0)

        if comm:
            for o, r in halo_pairs:
                t = lax.rem(s + r, 4)
                pltpu.make_async_remote_copy(
                    src_ref=sendb.at[o * 4 + t],
                    dst_ref=ghost.at[o * 4 + t],
                    send_sem=sem_fs.at[0],
                    recv_sem=sem_fr.at[o * 4 + t],
                    device_id=row_peer(o - 1, r),
                    device_id_type=MESH,
                ).wait_recv()

        def forward_faces(i, carry):
            at = pl.ds(pl.multiple_of(i * BLK, BLK), BLK)
            lo, hi = split_index(snd[:, at])
            total = stk[0:64, at].astype(f32)
            for pair in range(NB // 2):
                table = jnp.concatenate([ghost[2 * pair], ghost[2 * pair + 1]], axis=1)
                total = total + mm(table, selector(lo, hi, 4 + pair, iota2))
            stk[0:64, at] = total.astype(bf16)
            linear = mm(w1t[...], stk[0:192, at]) + wide(vec[0], BLK)
            gate = logistic(linear)
            active = (linear * gate).astype(bf16)
            stk[192:256, at] = active
            slope[:, at] = gate * (1.0 + linear * (1.0 - gate))
            scaled, spread = standardize(mm(w2t[...], active))
            scl[:, at] = scaled
            spr[:, at] = spread
            msg[:, at] = (scaled * wide(vec[1], BLK) + wide(vec[2], BLK)).astype(bf16)
            return carry

        lax.fori_loop(0, NF // BLK, forward_faces, 0)

        acc[:, 0:NC] = jnp.zeros((D, NC), f32)

        def sum_messages(i, carry):
            at = pl.ds(pl.multiple_of(i * BLK, BLK), BLK)
            lo, hi = col_r[at, 0:128], col_r[at, 128:256]
            part = msg[:, at]
            for tile in range(4):
                where = slice(256 * tile, 256 * tile + 256)
                acc[:, where] += mm(part, selector_t(lo, hi, tile, iotas))
            return carry

        lax.fori_loop(0, NF // BLK, sum_messages, 0)

        def cells(i, carry):
            at = pl.ds(pl.multiple_of(i * BLK, BLK), BLK)
            nin[64:128, at] = acc[:, at].astype(bf16)
            linear = mm(nw1t[...], nin[0:128, at]) + wide(vec[3], BLK)
            gate = logistic(linear)
            active = (linear * gate).astype(bf16)
            nin[128:192, at] = active
            scaled, spread = standardize(mm(nw2t[...], active))
            upstream = nct[:, at].astype(f32)
            sums[4] += fold_lanes(upstream * scaled)
            sums[5] += fold_lanes(upstream)
            delta = normalize_back(upstream, scaled, spread, wide(vec[4], BLK)).astype(bf16)
            nh2[0:64, at] = delta
            hidden = mm(nw2[...], delta) * (gate * (1.0 + linear * (1.0 - gate)))
            sums[3] += fold_lanes(hidden)
            hidden = hidden.astype(bf16)
            nh2[64:128, at] = hidden
            back = mm(nw1[...], hidden)
            own[:, at] = back[0:64] + upstream
            nbr[:, at] = back[64:128].astype(bf16)
            return carry

        lax.fori_loop(0, NC // BLK, cells, 0)

        def backward_faces(i, carry):
            at = pl.ds(pl.multiple_of(i * BLK, BLK), BLK)
            lo, hi = split_index(rcv[:, at])
            cotangent = ect[:, at].astype(f32)
            upstream = cotangent
            for tile in range(4):
                upstream = upstream + mm(
                    nbr[:, 256 * tile : 256 * tile + 256], selector(lo, hi, tile, iota2)
                )
            scaled = scl[:, at]
            sums[1] += fold_lanes(upstream * scaled)
            sums[2] += fold_lanes(upstream)
            delta = normalize_back(upstream, scaled, spr[:, at], wide(vec[1], BLK)).astype(bf16)
            ehd[64:128, at] = delta
            hidden = mm(w2[...], delta) * slope[:, at]
            sums[0] += fold_lanes(hidden)
            hidden = hidden.astype(bf16)
            ehd[0:64, at] = hidden
            dedges[:, at] = (cotangent + mm(w1[128:192, :], hidden)).astype(bf16)
            return carry

        lax.fori_loop(0, NF // BLK, backward_faces, 0)

        edge_part = mm_last(stk[...], ehd[...])
        node_part = mm_last(nin[...], nh2[...])
        lane64 = lax.broadcasted_iota(jnp.int32, (64, 128), 1)
        vectors = jnp.zeros((64, 128), f32)
        for number in range(6):
            vectors = jnp.where(
                lane64 == 64 + number, jnp.sum(sums[number], axis=1, keepdims=True), vectors
            )
        grads[0:64] = jnp.where(lane64 < 64, edge_part[0:64], node_part[0:64])
        grads[64:128] = jnp.where(lane64 < 64, edge_part[64:128], node_part[64:128])
        grads[128:192] = jnp.where(lane64 < 64, edge_part[128:192], vectors)
        grads[192:256] = jnp.where(lane64 < 64, node_part[128:192], edge_part[192:256])

        first = []
        if comm:
            for j in range(1, 8):
                other, peer = a_peer(j)
                first.append(
                    pltpu.make_async_remote_copy(
                        src_ref=grads.at[pl.ds(pl.multiple_of(other * 32, 32), 32), :],
                        dst_ref=rs_buf.at[a],
                        send_sem=sem_rs.at[j],
                        recv_sem=sem_rr.at[a],
                        device_id=peer,
                        device_id_type=MESH,
                    )
                )
            for copy in first:
                copy.start()

        acc[...] = jnp.zeros_like(acc)

        def sum_ghosts(i, carry):
            at = pl.ds(pl.multiple_of(i * BLK, BLK), BLK)
            lo, hi = col_s[at, 0:128], col_s[at, 128:256]
            part = ehd[0:64, at]
            for tile in range(6):
                where = slice(256 * tile, 256 * tile + 256)
                acc[:, where] += mm(part, selector_t(lo, hi, 4 + tile, iotas))
            return carry

        lax.fori_loop(0, NF // BLK, sum_ghosts, 0)
        for pair in range(NB // 2):
            block = mm(
                w1[0:64, :], acc[:, 256 * pair : 256 * pair + 256].astype(bf16)
            ).astype(bf16)
            gsend[2 * pair] = block[:, :HALO]
            gsend[2 * pair + 1] = block[:, HALO:]
        if comm:
            for number, (o, r) in enumerate(halo_pairs):
                t = lax.rem(s + r, 4)
                backward.append(
                    pltpu.make_async_remote_copy(
                        src_ref=gsend.at[o * 4 + t],
                        dst_ref=gback.at[o * 4 + s],
                        send_sem=sem_bs.at[number],
                        recv_sem=sem_br.at[o * 4 + s],
                        device_id=row_peer(1 - o, r),
                        device_id_type=MESH,
                    )
                )
            for copy in backward:
                copy.start()

        second = []
        if comm:
            total = grads[pl.ds(pl.multiple_of(a * 32, 32), 32), :]
            for j in range(1, 8):
                other, peer = a_peer(j)
                pltpu.make_async_remote_copy(
                    src_ref=rs_buf.at[other],
                    dst_ref=rs_buf.at[other],
                    send_sem=sem_rs.at[j],
                    recv_sem=sem_rr.at[other],
                    device_id=peer,
                    device_id_type=MESH,
                ).wait_recv()
                total = total + rs_buf[other]
            ex_buf[b] = total
            for j in range(1, 16):
                other, peer = b_peer(j)
                second.append(
                    pltpu.make_async_remote_copy(
                        src_ref=ex_buf.at[b],
                        dst_ref=ex_buf.at[b],
                        send_sem=sem_es.at[j],
                        recv_sem=sem_er.at[b],
                        device_id=peer,
                        device_id_type=MESH,
                    )
                )
            for copy in second:
                copy.start()

        acc[:, 0:NC] = jnp.zeros((D, NC), f32)
        gt[...] = jnp.zeros_like(gt)

        def sum_own(i, carry):
            at = pl.ds(pl.multiple_of(i * BLK, BLK), BLK)
            part = ehd[0:64, at]
            for cols, total in ((col_s, acc), (col_r, gt)):
                lo, hi = cols[at, 0:128], cols[at, 128:256]
                for tile in range(4):
                    where = slice(256 * tile, 256 * tile + 256)
                    total[:, where] += mm(part, selector_t(lo, hi, tile, iotas))
            return carry

        lax.fori_loop(0, NF // BLK, sum_own, 0)
        own[...] += mm(w1[0:64, :], acc[:, 0:NC].astype(bf16)) + mm(
            w1[64:128, :], gt[...].astype(bf16)
        )

        third = []
        if comm:
            for j in range(1, 16):
                other, peer = b_peer(j)
                pltpu.make_async_remote_copy(
                    src_ref=ex_buf.at[other],
                    dst_ref=ex_buf.at[other],
                    send_sem=sem_es.at[j],
                    recv_sem=sem_er.at[other],
                    device_id=peer,
                    device_id_type=MESH,
                ).wait_recv()
            total = ex_buf[0]
            for j in range(1, 16):
                total = total + ex_buf[j]
            ag_buf[a] = total
            for j in range(1, 8):
                other, peer = a_peer(j)
                third.append(
                    pltpu.make_async_remote_copy(
                        src_ref=ag_buf.at[a],
                        dst_ref=ag_buf.at[a],
                        send_sem=sem_as.at[j],
                        recv_sem=sem_ar.at[a],
                        device_id=peer,
                        device_id_type=MESH,
                    )
                )
            for copy in third:
                copy.start()

            for o, r in halo_pairs:
                t = lax.rem(s + r, 4)
                pltpu.make_async_remote_copy(
                    src_ref=gsend.at[o * 4 + t],
                    dst_ref=gback.at[o * 4 + t],
                    send_sem=sem_bs.at[0],
                    recv_sem=sem_br.at[o * 4 + t],
                    device_id=row_peer(1 - o, r),
                    device_id_type=MESH,
                ).wait_recv()

        returned = jnp.concatenate([gback[k] for k in range(NB)], axis=1)
        for tile in range(4):
            where = slice(256 * tile, 256 * tile + 256)
            total = own[:, where]
            for pair in range(NB // 2):
                at = slice(256 * pair, 256 * pair + 256)
                total = total + mm(
                    returned[:, at],
                    selector_t(col_p[at, 0:128], col_p[at, 128:256], tile, iotas),
                )
            dstate[:, where] = total.astype(bf16)

        if comm:
            for j in range(1, 8):
                other, peer = a_peer(j)
                pltpu.make_async_remote_copy(
                    src_ref=ag_buf.at[other],
                    dst_ref=ag_buf.at[other],
                    send_sem=sem_as.at[j],
                    recv_sem=sem_ar.at[other],
                    device_id=peer,
                    device_id_type=MESH,
                ).wait_recv()
            whole = jnp.concatenate([ag_buf[j] for j in range(8)], axis=0) * FACTOR
        else:
            whole = grads[...] * FACTOR
        o_w1[...] = whole[0:192, 0:64]
        o_nw2[...] = whole[192:256, 0:64]
        swapped = jnp.concatenate([whole[0:128], whole[192:256]], axis=0)
        swapped = pltpu.roll(swapped, 64, 1)
        o_nw1[...] = swapped[0:128, 0:64]
        o_w2[...] = swapped[128:192, 0:64]
        rows = whole[128:192, :].T
        o_b1[...] = rows[64:65, :]
        o_eg[...] = rows[65:66, :]
        o_es[...] = rows[66:67, :]
        o_nb1[...] = rows[67:68, :]
        o_ng[...] = rows[68:69, :]
        o_ns[...] = rows[69:70, :]
        for copy in forward + backward + first + second + third:
            copy.wait_send()

    return kernel


def call(comm, *args):
    shapes = [
        ((D, NC), bf16),
        ((D, NF), bf16),
        ((192, 64), f32),
        ((1, 64), f32),
        ((64, 64), f32),
        ((1, 64), f32),
        ((1, 64), f32),
        ((128, 64), f32),
        ((1, 64), f32),
        ((64, 64), f32),
        ((1, 64), f32),
        ((1, 64), f32),
    ]
    dma = pltpu.SemaphoreType.DMA
    scratch = [
        pltpu.VMEM((256, NF), bf16),
        pltpu.VMEM((D, NF), f32),
        pltpu.VMEM((D, NF), f32),
        pltpu.VMEM((1, NF), f32),
        pltpu.VMEM((D, NF), bf16),
        pltpu.VMEM((128, NF), bf16),
        pltpu.VMEM((NF, 256), bf16),
        pltpu.VMEM((NF, 256), bf16),
        pltpu.VMEM((NB * HALO, 256), bf16),
        pltpu.VMEM((NB, D, HALO), bf16),
        pltpu.VMEM((NB, D, HALO), bf16),
        pltpu.VMEM((NB, D, HALO), bf16),
        pltpu.VMEM((NB, D, HALO), bf16),
        pltpu.VMEM((192, NC), bf16),
        pltpu.VMEM((128, NC), bf16),
        pltpu.VMEM((D, NC), bf16),
        pltpu.VMEM((D, NC), f32),
        pltpu.VMEM((D, NB * HALO), f32),
        pltpu.VMEM((D, NC), f32),
        pltpu.VMEM((D, HALO), bf16),
        pltpu.VMEM((5, D, 128), f32),
        pltpu.VMEM((6, D, 128), f32),
        pltpu.VMEM((256, 128), f32),
        pltpu.VMEM((8, 32, 128), f32),
        pltpu.VMEM((16, 32, 128), f32),
        pltpu.VMEM((8, 32, 128), f32),
        pltpu.VMEM((64, 192), bf16),
        pltpu.VMEM((64, 64), bf16),
        pltpu.VMEM((64, 128), bf16),
        pltpu.VMEM((64, 64), bf16),
        dma((12,)), dma((12,)), dma((12,)), dma((12,)),
        dma((8,)), dma((8,)), dma((16,)), dma((16,)), dma((8,)), dma((8,)),
    ]
    vmem = pl.BlockSpec(memory_space=pltpu.VMEM)
    params = dict(vmem_limit_bytes=48 * 1024 * 1024)
    if comm:
        params.update(collective_id=0, has_side_effects=True)
    return pl.pallas_call(
        make_kernel(comm),
        out_shape=[jax.ShapeDtypeStruct(shape, kind) for shape, kind in shapes],
        in_specs=[vmem] * 16,
        out_specs=[vmem] * 12,
        scratch_shapes=scratch,
        compiler_params=pltpu.CompilerParams(**params),
        name="layer",
    )(*args)


def on_device(comm, node_state, edge_state, senders, receivers, send_index, node_cotangent, edge_cotangent,
              edge_first, edge_bias, edge_second, edge_gain, edge_shift, node_first, node_bias, node_second, node_gain):
    line = lambda v: v.reshape(1, -1)
    outs = call(
        comm, node_state, edge_state, line(senders), line(receivers), send_index.reshape(NB, HALO),
        node_cotangent, edge_cotangent, edge_first, line(edge_bias), edge_second, line(edge_gain),
        line(edge_shift), node_first, line(node_bias), node_second, line(node_gain),
    )
    return tuple(v.reshape(-1) if v.shape[0] == 1 else v for v in outs)


def solution(mesh):
    split = Mesh(mesh.devices.reshape(4, 4, 2, 4), AXES)
    every = P(None, AXES)
    in_specs = (every, every, P(AXES), P(AXES), P(AXES, None, None), every, every) + (P(),) * 9
    out_specs = (every, every) + (P(),) * 10
    return jax.shard_map(
        lambda *args: on_device(True, *args), mesh=split, in_specs=in_specs, out_specs=out_specs,
        check_vma=False,
    )
```

```python
import math

import jax
import jax.numpy as jnp
from jax import lax
from jax.experimental import pallas as pl
from jax.experimental.pallas import tpu as pltpu
from jax.sharding import Mesh
from jax.sharding import PartitionSpec as P

AXES = ("z", "y", "core", "sub")
MESH = pl.DeviceIdType.MESH
EPSILON = 1e-05
D = 64
NF = 3072
NC = 1024
NB = 12
HALO = 128
BLK = 512
bf16 = jnp.bfloat16
f32 = jnp.float32
FACTOR = 1.0 / math.sqrt(393216)


def mm(a, b):
    return jnp.dot(a, b, preferred_element_type=f32)


def mm_last(a, b):
    return lax.dot_general(a, b, (((1,), (1,)), ((), ())), preferred_element_type=f32)


def split_index(row):
    return row & 255, row >> 8


def sub_iota(width):
    return lax.broadcasted_iota(jnp.int32, (256, width), 0).astype(f32).astype(bf16)


def selector(lo, hi, tile, iota):
    key = jnp.where(hi == tile, lo, -1).astype(f32).astype(bf16)
    return jnp.where(iota == key, bf16(1), bf16(0))


def columns_of(lo, hi):
    width = lo.shape[1]
    row = lax.broadcasted_iota(jnp.int32, (8, width), 0)
    stacked = jnp.where(row == 0, lo, jnp.where(row == 1, hi, 0)).astype(f32)
    sub = lax.broadcasted_iota(jnp.int32, (8, 256), 0)
    lane = lax.broadcasted_iota(jnp.int32, (8, 256), 1)
    chooser = jnp.where(((sub == 0) & (lane < 128)) | ((sub == 1) & (lane >= 128)), 1.0, 0.0)
    out = lax.dot_general(
        stacked, chooser, (((0,), (0,)), ((), ())), preferred_element_type=f32
    )
    return out.astype(bf16)


def lane_iotas():
    lane = lax.broadcasted_iota(jnp.int32, (1, 128), 1)
    return lane.astype(f32).astype(bf16), (lane + 128).astype(f32).astype(bf16)


def selector_t(lo, hi, tile, iotas):
    key = jnp.where(hi == bf16(tile), lo, bf16(-1))
    return jnp.concatenate(
        [jnp.where(key == lanes, bf16(1), bf16(0)) for lanes in iotas], axis=1
    )


def column_of(row):
    sub = lax.broadcasted_iota(jnp.int32, (D, D), 0)
    lane = lax.broadcasted_iota(jnp.int32, (D, D), 1)
    col = jnp.sum(jnp.where(sub == lane, row, 0.0), axis=1, keepdims=True)
    return jnp.broadcast_to(col, (D, 128))


def wide(col, width):
    return jnp.concatenate([col] * (width // 128), axis=1)


def fold_lanes(values):
    total = values[:, 0:128]
    for begin in range(128, values.shape[1], 128):
        total = total + values[:, begin : begin + 128]
    return total


def mean_rows(values):
    return jnp.sum(values, axis=0, keepdims=True) * (1.0 / D)


def logistic(values):
    return 0.5 * jnp.tanh(0.5 * values) + 0.5


def standardize(values):
    centered = values - mean_rows(values)
    spread = lax.rsqrt(mean_rows(centered * centered) + EPSILON)
    return centered * spread, spread


def normalize_back(upstream, scaled, spread, gain):
    weighted = upstream * gain
    return spread * (weighted - mean_rows(weighted) - scaled * mean_rows(weighted * scaled))


def make_kernel(comm):
    def kernel(
        *refs
    ):
        given, refs = refs[:16], refs[16:]
        (dstate, dedges, packed), refs = refs[:3], refs[3:]
        held, refs = refs[:16], refs[16:]
        (
            stk, slope, scl, spr, msg, ehd, col_s, col_r, col_p,
            sendb, ghost, gsend, gback, nin, nh2, nbr, own, acc, gt, gsb,
            vec, sums, grads, rs_buf, ex_buf, ag_buf, w1, w2t, nw1, nw2t,
            sem_fs, sem_fr, sem_bs, sem_br, sem_rs, sem_rr, sem_es, sem_er, sem_as, sem_ar,
            sem_in,
        ) = refs
        ns, es, snd, rcv, six, nct, ect, w1t, b1, w2, eg, esh, nw1t, nb1, nw2, ng = held
        loads = [
            pltpu.make_async_copy(given[k], held[k], sem_in.at[k]) for k in range(16)
        ]
        for k in (4, 0, 2, 3, 1, 7, 8, 9, 10, 11, 12, 13, 14, 15, 5, 6):
            loads[k].start()
        if comm:
            z = lax.axis_index("z")
            y = lax.axis_index("y")
            core = lax.axis_index("core")
            s = lax.axis_index("sub")
            d = z * 8 + y * 2 + core
            a = z * 2 + core
            b = y * 4 + s

            def row_peer(step, r):
                dd = lax.rem(d + (step + 32), 32)
                return (
                    lax.div(dd, 8),
                    lax.rem(lax.div(dd, 2), 4),
                    lax.rem(dd, 2),
                    lax.rem(s + r, 4),
                )

            def a_peer(j):
                other = lax.rem(a + j, 8)
                return other, (lax.div(other, 2), y, lax.rem(other, 2), s)

            def b_peer(j):
                other = lax.rem(b + j, 16)
                return other, (z, lax.div(other, 4), core, lax.rem(other, 4))

            halo_pairs = [(o, r) for o in range(3) for r in range(4) if not (o == 1 and r == 0)]
            barrier = pltpu.get_barrier_semaphore()
            peers = [row_peer(o - 1, r) for o, r in halo_pairs]
            peers += [a_peer(j)[1] for j in range(1, 8)] + [b_peer(j)[1] for j in range(1, 16)]
            for peer in peers:
                pl.semaphore_signal(barrier, inc=1, device_id=peer, device_id_type=MESH)
        else:
            s = 0

        iota = sub_iota(256)
        iota2 = jnp.concatenate([iota, iota], axis=1)
        iotas = lane_iotas()

        loads[4].wait()
        loads[0].wait()
        for pair in range(NB // 2):
            row = six[:, 256 * pair : 256 * pair + 256]
            lo, hi = split_index(row)
            picked = jnp.zeros((D, 256), f32)
            for tile in range(4):
                picked = picked + mm(
                    ns[:, 256 * tile : 256 * tile + 256], selector(lo, hi, tile, iota)
                )
            picked = picked.astype(bf16)
            sendb[2 * pair] = picked[:, :HALO]
            sendb[2 * pair + 1] = picked[:, HALO:]
            col_p[256 * pair : 256 * pair + 256, :] = columns_of(lo, hi)

        ghost[4 + s] = jnp.zeros((D, HALO), bf16)
        gback[4 + s] = jnp.zeros((D, HALO), bf16)

        forward = []
        backward = []
        if comm:
            pl.semaphore_wait(barrier, len(peers))
            for number, (o, r) in enumerate(halo_pairs):
                t = lax.rem(s + r, 4)
                forward.append(
                    pltpu.make_async_remote_copy(
                        src_ref=sendb.at[o * 4 + t],
                        dst_ref=ghost.at[o * 4 + s],
                        send_sem=sem_fs.at[number],
                        recv_sem=sem_fr.at[o * 4 + s],
                        device_id=row_peer(o - 1, r),
                        device_id_type=MESH,
                    )
                )
            for copy in forward:
                copy.start()

        for k in (2, 3, 1, 7, 8, 9, 10, 11, 12, 13, 14, 15):
            loads[k].wait()
        vec[0] = column_of(b1[...])
        vec[1] = column_of(eg[...])
        vec[2] = column_of(esh[...])
        vec[3] = column_of(nb1[...])
        vec[4] = column_of(ng[...])
        w1[...] = w1t[...].astype(f32).T.astype(bf16)
        w2t[...] = w2[...].astype(f32).T.astype(bf16)
        nw1[...] = nw1t[...].astype(f32).T.astype(bf16)
        nw2t[...] = nw2[...].astype(f32).T.astype(bf16)
        sums[...] = jnp.zeros_like(sums)
        stk[128:192, :] = es[...]
        nin[0:64, :] = ns[...]

        def gather_own(i, carry):
            at = pl.ds(pl.multiple_of(i * BLK, BLK), BLK)
            for index, begin, cols in ((snd, 0, col_s), (rcv, 64, col_r)):
                lo, hi = split_index(index[:, at])
                total = jnp.zeros((D, BLK), f32)
                for tile in range(4):
                    total = total + mm(
                        ns[:, 256 * tile : 256 * tile + 256], selector(lo, hi, tile, iota2)
                    )
                stk[begin : begin + 64, at] = total.astype(bf16)
                cols[at, :] = columns_of(lo, hi)
            return carry

        lax.fori_loop(0, NF // BLK, gather_own, 0)

        if comm:
            for o, r in halo_pairs:
                t = lax.rem(s + r, 4)
                pltpu.make_async_remote_copy(
                    src_ref=sendb.at[o * 4 + t],
                    dst_ref=ghost.at[o * 4 + t],
                    send_sem=sem_fs.at[0],
                    recv_sem=sem_fr.at[o * 4 + t],
                    device_id=row_peer(o - 1, r),
                    device_id_type=MESH,
                ).wait_recv()

        def forward_faces(i, carry):
            at = pl.ds(pl.multiple_of(i * BLK, BLK), BLK)
            lo, hi = split_index(snd[:, at])
            total = stk[0:64, at].astype(f32)
            for pair in range(NB // 2):
                table = jnp.concatenate([ghost[2 * pair], ghost[2 * pair + 1]], axis=1)
                total = total + mm(table, selector(lo, hi, 4 + pair, iota2))
            stk[0:64, at] = total.astype(bf16)
            linear = mm(w1t[...], stk[0:192, at]) + wide(vec[0], BLK)
            gate = logistic(linear)
            active = (linear * gate).astype(bf16)
            stk[192:256, at] = active
            slope[:, at] = gate * (1.0 + linear * (1.0 - gate))
            scaled, spread = standardize(mm(w2t[...], active))
            scl[:, at] = scaled
            spr[:, at] = spread
            msg[:, at] = (scaled * wide(vec[1], BLK) + wide(vec[2], BLK)).astype(bf16)
            return carry

        lax.fori_loop(0, NF // BLK, forward_faces, 0)

        acc[:, 0:NC] = jnp.zeros((D, NC), f32)

        def sum_messages(i, carry):
            at = pl.ds(pl.multiple_of(i * BLK, BLK), BLK)
            lo, hi = col_r[at, 0:128], col_r[at, 128:256]
            part = msg[:, at]
            for tile in range(4):
                where = slice(256 * tile, 256 * tile + 256)
                acc[:, where] += mm(part, selector_t(lo, hi, tile, iotas))
            return carry

        lax.fori_loop(0, NF // BLK, sum_messages, 0)

        loads[5].wait()
        loads[6].wait()
        def cells(i, carry):
            at = pl.ds(pl.multiple_of(i * BLK, BLK), BLK)
            nin[64:128, at] = acc[:, at].astype(bf16)
            linear = mm(nw1t[...], nin[0:128, at]) + wide(vec[3], BLK)
            gate = logistic(linear)
            active = (linear * gate).astype(bf16)
            nin[128:192, at] = active
            scaled, spread = standardize(mm(nw2t[...], active))
            upstream = nct[:, at].astype(f32)
            sums[4] += fold_lanes(upstream * scaled)
            sums[5] += fold_lanes(upstream)
            delta = normalize_back(upstream, scaled, spread, wide(vec[4], BLK)).astype(bf16)
            nh2[0:64, at] = delta
            hidden = mm(nw2[...], delta) * (gate * (1.0 + linear * (1.0 - gate)))
            sums[3] += fold_lanes(hidden)
            hidden = hidden.astype(bf16)
            nh2[64:128, at] = hidden
            back = mm(nw1[...], hidden)
            own[:, at] = back[0:64] + upstream
            nbr[:, at] = back[64:128].astype(bf16)
            return carry

        lax.fori_loop(0, NC // BLK, cells, 0)

        def backward_faces(i, carry):
            at = pl.ds(pl.multiple_of(i * BLK, BLK), BLK)
            lo, hi = split_index(rcv[:, at])
            cotangent = ect[:, at].astype(f32)
            upstream = cotangent
            for tile in range(4):
                upstream = upstream + mm(
                    nbr[:, 256 * tile : 256 * tile + 256], selector(lo, hi, tile, iota2)
                )
            scaled = scl[:, at]
            sums[1] += fold_lanes(upstream * scaled)
            sums[2] += fold_lanes(upstream)
            delta = normalize_back(upstream, scaled, spr[:, at], wide(vec[1], BLK)).astype(bf16)
            ehd[64:128, at] = delta
            hidden = mm(w2[...], delta) * slope[:, at]
            sums[0] += fold_lanes(hidden)
            hidden = hidden.astype(bf16)
            ehd[0:64, at] = hidden
            dedges[:, at] = (cotangent + mm(w1[128:192, :], hidden)).astype(bf16)
            return carry

        lax.fori_loop(0, NF // BLK, backward_faces, 0)

        edge_part = mm_last(stk[...], ehd[...])
        node_part = mm_last(nin[...], nh2[...])
        lane64 = lax.broadcasted_iota(jnp.int32, (64, 128), 1)
        vectors = jnp.zeros((64, 128), f32)
        for number in range(6):
            vectors = jnp.where(
                lane64 == 64 + number, jnp.sum(sums[number], axis=1, keepdims=True), vectors
            )
        grads[0:64] = jnp.where(lane64 < 64, edge_part[0:64], node_part[0:64])
        grads[64:128] = jnp.where(lane64 < 64, edge_part[64:128], node_part[64:128])
        grads[128:192] = jnp.where(lane64 < 64, edge_part[128:192], vectors)
        grads[192:256] = jnp.where(lane64 < 64, node_part[128:192], edge_part[192:256])

        first = []
        if comm:
            for j in range(1, 8):
                other, peer = a_peer(j)
                first.append(
                    pltpu.make_async_remote_copy(
                        src_ref=grads.at[pl.ds(pl.multiple_of(other * 32, 32), 32), :],
                        dst_ref=rs_buf.at[a],
                        send_sem=sem_rs.at[j],
                        recv_sem=sem_rr.at[a],
                        device_id=peer,
                        device_id_type=MESH,
                    )
                )
            for copy in first:
                copy.start()

        acc[...] = jnp.zeros_like(acc)

        def sum_ghosts(i, carry):
            at = pl.ds(pl.multiple_of(i * BLK, BLK), BLK)
            lo, hi = col_s[at, 0:128], col_s[at, 128:256]
            part = ehd[0:64, at]
            for tile in range(6):
                where = slice(256 * tile, 256 * tile + 256)
                acc[:, where] += mm(part, selector_t(lo, hi, 4 + tile, iotas))
            return carry

        lax.fori_loop(0, NF // BLK, sum_ghosts, 0)
        for pair in range(NB // 2):
            block = mm(
                w1[0:64, :], acc[:, 256 * pair : 256 * pair + 256].astype(bf16)
            ).astype(bf16)
            gsend[2 * pair] = block[:, :HALO]
            gsend[2 * pair + 1] = block[:, HALO:]
        if comm:
            for number, (o, r) in enumerate(halo_pairs):
                t = lax.rem(s + r, 4)
                backward.append(
                    pltpu.make_async_remote_copy(
                        src_ref=gsend.at[o * 4 + t],
                        dst_ref=gback.at[o * 4 + s],
                        send_sem=sem_bs.at[number],
                        recv_sem=sem_br.at[o * 4 + s],
                        device_id=row_peer(1 - o, r),
                        device_id_type=MESH,
                    )
                )
            for copy in backward:
                copy.start()

        second = []
        if comm:
            total = grads[pl.ds(pl.multiple_of(a * 32, 32), 32), :]
            for j in range(1, 8):
                other, peer = a_peer(j)
                pltpu.make_async_remote_copy(
                    src_ref=rs_buf.at[other],
                    dst_ref=rs_buf.at[other],
                    send_sem=sem_rs.at[j],
                    recv_sem=sem_rr.at[other],
                    device_id=peer,
                    device_id_type=MESH,
                ).wait_recv()
                total = total + rs_buf[other]
            ex_buf[b] = total
            for j in range(1, 16):
                other, peer = b_peer(j)
                second.append(
                    pltpu.make_async_remote_copy(
                        src_ref=ex_buf.at[b],
                        dst_ref=ex_buf.at[b],
                        send_sem=sem_es.at[j],
                        recv_sem=sem_er.at[b],
                        device_id=peer,
                        device_id_type=MESH,
                    )
                )
            for copy in second:
                copy.start()

        acc[:, 0:NC] = jnp.zeros((D, NC), f32)
        gt[...] = jnp.zeros_like(gt)

        def sum_own(i, carry):
            at = pl.ds(pl.multiple_of(i * BLK, BLK), BLK)
            part = ehd[0:64, at]
            for cols, total in ((col_s, acc), (col_r, gt)):
                lo, hi = cols[at, 0:128], cols[at, 128:256]
                for tile in range(4):
                    where = slice(256 * tile, 256 * tile + 256)
                    total[:, where] += mm(part, selector_t(lo, hi, tile, iotas))
            return carry

        lax.fori_loop(0, NF // BLK, sum_own, 0)
        own[...] += mm(w1[0:64, :], acc[:, 0:NC].astype(bf16)) + mm(
            w1[64:128, :], gt[...].astype(bf16)
        )

        third = []
        if comm:
            for j in range(1, 16):
                other, peer = b_peer(j)
                pltpu.make_async_remote_copy(
                    src_ref=ex_buf.at[other],
                    dst_ref=ex_buf.at[other],
                    send_sem=sem_es.at[j],
                    recv_sem=sem_er.at[other],
                    device_id=peer,
                    device_id_type=MESH,
                ).wait_recv()
            total = ex_buf[0]
            for j in range(1, 16):
                total = total + ex_buf[j]
            ag_buf[a] = total
            for j in range(1, 8):
                other, peer = a_peer(j)
                third.append(
                    pltpu.make_async_remote_copy(
                        src_ref=ag_buf.at[a],
                        dst_ref=ag_buf.at[a],
                        send_sem=sem_as.at[j],
                        recv_sem=sem_ar.at[a],
                        device_id=peer,
                        device_id_type=MESH,
                    )
                )
            for copy in third:
                copy.start()

            for o, r in halo_pairs:
                t = lax.rem(s + r, 4)
                pltpu.make_async_remote_copy(
                    src_ref=gsend.at[o * 4 + t],
                    dst_ref=gback.at[o * 4 + t],
                    send_sem=sem_bs.at[0],
                    recv_sem=sem_br.at[o * 4 + t],
                    device_id=row_peer(1 - o, r),
                    device_id_type=MESH,
                ).wait_recv()

        returned = jnp.concatenate([gback[k] for k in range(NB)], axis=1)
        for tile in range(4):
            where = slice(256 * tile, 256 * tile + 256)
            total = own[:, where]
            for pair in range(NB // 2):
                at = slice(256 * pair, 256 * pair + 256)
                total = total + mm(
                    returned[:, at],
                    selector_t(col_p[at, 0:128], col_p[at, 128:256], tile, iotas),
                )
            dstate[:, where] = total.astype(bf16)

        if comm:
            for j in range(1, 8):
                other, peer = a_peer(j)
                pltpu.make_async_remote_copy(
                    src_ref=ag_buf.at[other],
                    dst_ref=ag_buf.at[other],
                    send_sem=sem_as.at[j],
                    recv_sem=sem_ar.at[other],
                    device_id=peer,
                    device_id_type=MESH,
                ).wait_recv()
            for j in range(8):
                packed[32 * j : 32 * j + 32] = ag_buf[j]
        else:
            packed[...] = grads[...]
        for copy in forward + backward + first + second + third:
            copy.wait_send()

    return kernel


def finish(
    dstate, dedges, packed, out_state, out_edges, *refs
):
    results, refs = refs[:10], refs[10:]
    staged, sems = refs[:10], refs[10]
    o_w1, o_b1, o_w2, o_eg, o_es, o_nw1, o_nb1, o_nw2, o_ng, o_ns = staged
    stores = [
        pltpu.make_async_copy(dedges, out_edges, sems.at[10]),
        pltpu.make_async_copy(dstate, out_state, sems.at[11]),
    ]
    for copy in stores:
        copy.start()
    whole = packed[...] * FACTOR
    turned = jnp.concatenate([whole[0:128].T, whole[128:256].T], axis=1)
    o_w1[...] = turned[0:64, 0:192]
    o_nw1[...] = turned[64:128, 0:128]
    o_nw2[...] = whole[192:256, 0:64]
    o_w2[...] = pltpu.roll(whole[192:256], 64, 1)[:, 0:64]
    rows = turned[64:128, 128:192]
    for k, ref in enumerate((o_b1, o_eg, o_es, o_nb1, o_ng, o_ns)):
        ref[...] = rows[k : k + 1, :]
    for k in range(10):
        copy = pltpu.make_async_copy(staged[k], results[k], sems.at[k])
        copy.start()
        stores.append(copy)
    for copy in stores:
        copy.wait()


def call(comm, *args):
    shapes = [
        ((D, NC), bf16),
        ((D, NF), bf16),
        ((64, 192), f32),
        ((1, 64), f32),
        ((64, 64), f32),
        ((1, 64), f32),
        ((1, 64), f32),
        ((64, 128), f32),
        ((1, 64), f32),
        ((64, 64), f32),
        ((1, 64), f32),
        ((1, 64), f32),
    ]
    dma = pltpu.SemaphoreType.DMA
    scratch = [pltpu.VMEM(arg.shape, arg.dtype) for arg in args]
    scratch += [
        pltpu.VMEM((256, NF), bf16),
        pltpu.VMEM((D, NF), f32),
        pltpu.VMEM((D, NF), f32),
        pltpu.VMEM((1, NF), f32),
        pltpu.VMEM((D, NF), bf16),
        pltpu.VMEM((128, NF), bf16),
        pltpu.VMEM((NF, 256), bf16),
        pltpu.VMEM((NF, 256), bf16),
        pltpu.VMEM((NB * HALO, 256), bf16),
        pltpu.VMEM((NB, D, HALO), bf16),
        pltpu.VMEM((NB, D, HALO), bf16),
        pltpu.VMEM((NB, D, HALO), bf16),
        pltpu.VMEM((NB, D, HALO), bf16),
        pltpu.VMEM((192, NC), bf16),
        pltpu.VMEM((128, NC), bf16),
        pltpu.VMEM((D, NC), bf16),
        pltpu.VMEM((D, NC), f32),
        pltpu.VMEM((D, NB * HALO), f32),
        pltpu.VMEM((D, NC), f32),
        pltpu.VMEM((D, HALO), bf16),
        pltpu.VMEM((5, D, 128), f32),
        pltpu.VMEM((6, D, 128), f32),
        pltpu.VMEM((256, 128), f32),
        pltpu.VMEM((8, 32, 128), f32),
        pltpu.VMEM((16, 32, 128), f32),
        pltpu.VMEM((8, 32, 128), f32),
        pltpu.VMEM((192, 64), bf16),
        pltpu.VMEM((64, 64), bf16),
        pltpu.VMEM((128, 64), bf16),
        pltpu.VMEM((64, 64), bf16),
        dma((12,)), dma((12,)), dma((12,)), dma((12,)),
        dma((8,)), dma((8,)), dma((16,)), dma((16,)), dma((8,)), dma((8,)),
        dma((16,)),
    ]
    anywhere = pl.BlockSpec(memory_space=pltpu.HBM)
    params = dict(vmem_limit_bytes=36 * 1024 * 1024)
    if comm:
        params.update(collective_id=0, has_side_effects=True)
    vmem = pl.BlockSpec(memory_space=pltpu.VMEM)
    middle = pl.pallas_call(
        make_kernel(comm),
        out_shape=[
            jax.ShapeDtypeStruct(shape, kind) for shape, kind in shapes[:2] + [((256, 128), f32)]
        ],
        in_specs=[anywhere] * 16,
        out_specs=[vmem] * 3,
        scratch_shapes=scratch,
        compiler_params=pltpu.CompilerParams(**params),
        name="layer",
    )(*args)
    return pl.pallas_call(
        finish,
        out_shape=[jax.ShapeDtypeStruct(shape, kind) for shape, kind in shapes],
        in_specs=[vmem] * 3,
        out_specs=[anywhere] * 12,
        scratch_shapes=[pltpu.VMEM(shape, kind) for shape, kind in shapes[2:]] + [dma((12,))],
        compiler_params=pltpu.CompilerParams(vmem_limit_bytes=8 * 1024 * 1024),
        name="finish",
    )(*middle)


def on_device(comm, node_state, edge_state, senders, receivers, send_index, node_cotangent, edge_cotangent,
              edge_first, edge_bias, edge_second, edge_gain, edge_shift, node_first, node_bias, node_second, node_gain):
    line = lambda v: v.reshape(1, -1)
    outs = call(
        comm, node_state, edge_state, line(senders), line(receivers), line(send_index),
        node_cotangent, edge_cotangent, edge_first.T, line(edge_bias), edge_second, line(edge_gain),
        line(edge_shift), node_first.T, line(node_bias), node_second, line(node_gain),
    )
    outs = [v.reshape(-1) if v.shape[0] == 1 else v for v in outs]
    outs[2] = outs[2].T
    outs[7] = outs[7].T
    return tuple(outs)


def solution(mesh):
    split = Mesh(mesh.devices.reshape(4, 4, 2, 4), AXES)
    every = P(None, AXES)
    in_specs = (every, every, P(AXES), P(AXES), P(AXES, None, None), every, every) + (P(),) * 9
    out_specs = (every, every) + (P(),) * 10
    return jax.shard_map(
        lambda *args: on_device(True, *args), mesh=split, in_specs=in_specs, out_specs=out_specs,
        check_vma=False,
    )
```

```python
import math

import jax
import jax.numpy as jnp
from jax import lax
from jax.experimental import pallas as pl
from jax.experimental.pallas import tpu as pltpu
from jax.sharding import Mesh
from jax.sharding import PartitionSpec as P

AXES = ("z", "y", "core", "sub")
MESH = pl.DeviceIdType.MESH
EPSILON = 1e-05
D = 64
NF = 3072
NC = 1024
NB = 12
HALO = 128
BLK = 512
bf16 = jnp.bfloat16
f32 = jnp.float32
FACTOR = 1.0 / math.sqrt(393216)


def mm(a, b):
    return jnp.dot(a, b, preferred_element_type=f32)


def mm_last(a, b):
    return lax.dot_general(a, b, (((1,), (1,)), ((), ())), preferred_element_type=f32)


def split_index(row):
    return row & 255, row >> 8


def sub_iota(width):
    return lax.broadcasted_iota(jnp.int32, (256, width), 0).astype(f32).astype(bf16)


def selector(lo, hi, tile, iota):
    key = jnp.where(hi == tile, lo, -1).astype(f32).astype(bf16)
    return jnp.where(iota == key, bf16(1), bf16(0))


def columns_of(lo, hi):
    width = lo.shape[1]
    row = lax.broadcasted_iota(jnp.int32, (8, width), 0)
    stacked = jnp.where(row == 0, lo, jnp.where(row == 1, hi, 0)).astype(f32)
    sub = lax.broadcasted_iota(jnp.int32, (8, 256), 0)
    lane = lax.broadcasted_iota(jnp.int32, (8, 256), 1)
    chooser = jnp.where(((sub == 0) & (lane < 128)) | ((sub == 1) & (lane >= 128)), 1.0, 0.0)
    out = lax.dot_general(
        stacked, chooser, (((0,), (0,)), ((), ())), preferred_element_type=f32
    )
    return out.astype(bf16)


def lane_iotas():
    lane = lax.broadcasted_iota(jnp.int32, (1, 128), 1)
    return lane.astype(f32).astype(bf16), (lane + 128).astype(f32).astype(bf16)


def selector_t(lo, hi, tile, iotas):
    key = jnp.where(hi == bf16(tile), lo, bf16(-1))
    return jnp.concatenate(
        [jnp.where(key == lanes, bf16(1), bf16(0)) for lanes in iotas], axis=1
    )


def column_of(row):
    sub = lax.broadcasted_iota(jnp.int32, (D, D), 0)
    lane = lax.broadcasted_iota(jnp.int32, (D, D), 1)
    col = jnp.sum(jnp.where(sub == lane, row, 0.0), axis=1, keepdims=True)
    return jnp.broadcast_to(col, (D, 128))


def wide(col, width):
    return jnp.concatenate([col] * (width // 128), axis=1)


def fold_lanes(values):
    total = values[:, 0:128]
    for begin in range(128, values.shape[1], 128):
        total = total + values[:, begin : begin + 128]
    return total


def mean_rows(values):
    return jnp.sum(values, axis=0, keepdims=True) * (1.0 / D)


def logistic(values):
    return 0.5 * jnp.tanh(0.5 * values) + 0.5


def standardize(values):
    centered = values - mean_rows(values)
    spread = lax.rsqrt(mean_rows(centered * centered) + EPSILON)
    return centered * spread, spread


def normalize_back(upstream, scaled, spread, gain):
    weighted = upstream * gain
    return spread * (weighted - mean_rows(weighted) - scaled * mean_rows(weighted * scaled))


def make_kernel(comm):
    def kernel(
        *refs
    ):
        given, refs = refs[:16], refs[16:]
        (dstate, dedges, packed), refs = refs[:3], refs[3:]
        held, refs = refs[:16], refs[16:]
        (
            stk, slope, scl, spr, msg, ehd, col_s, col_r, col_p,
            sendb, ghost, gsend, gback, nin, nh2, nbr, own, acc, gt, gsb,
            vec, sums, grads, rs_buf, ex_buf, ag_buf, w1, w2t, nw1, nw2t,
            sem_fs, sem_fr, sem_bs, sem_br, sem_rs, sem_rr, sem_es, sem_er, sem_as, sem_ar,
            sem_in,
        ) = refs
        ns, es, snd, rcv, six, nct, ect, w1t, b1, w2, eg, esh, nw1t, nb1, nw2, ng = held
        loads = [
            pltpu.make_async_copy(given[k], held[k], sem_in.at[k]) for k in range(16)
        ]
        for k in (4, 0, 2, 3, 1, 7, 8, 9, 10, 11, 12, 13, 14, 15, 5, 6):
            loads[k].start()
        if comm:
            z = lax.axis_index("z")
            y = lax.axis_index("y")
            core = lax.axis_index("core")
            s = lax.axis_index("sub")
            d = z * 8 + y * 2 + core
            a = z * 2 + core
            b = y * 4 + s

            def row_peer(step, r):
                dd = lax.rem(d + (step + 32), 32)
                return (
                    lax.div(dd, 8),
                    lax.rem(lax.div(dd, 2), 4),
                    lax.rem(dd, 2),
                    lax.rem(s + r, 4),
                )

            def a_peer(j):
                other = lax.rem(a + j, 8)
                return other, (lax.div(other, 2), y, lax.rem(other, 2), s)

            def b_peer(j):
                other = lax.rem(b + j, 16)
                return other, (z, lax.div(other, 4), core, lax.rem(other, 4))

            halo_pairs = [(o, r) for o in range(3) for r in range(4) if not (o == 1 and r == 0)]
            barrier = pltpu.get_barrier_semaphore()
            peers = [row_peer(o - 1, r) for o, r in halo_pairs]
            peers += [a_peer(j)[1] for j in range(1, 8)] + [b_peer(j)[1] for j in range(1, 16)]
            for peer in peers:
                pl.semaphore_signal(barrier, inc=1, device_id=peer, device_id_type=MESH)
        else:
            s = 0

        iota = sub_iota(256)
        iota2 = jnp.concatenate([iota, iota], axis=1)
        iotas = lane_iotas()

        loads[4].wait()
        loads[0].wait()
        for pair in range(NB // 2):
            row = six[:, 256 * pair : 256 * pair + 256]
            lo, hi = split_index(row)
            picked = jnp.zeros((D, 256), f32)
            for tile in range(4):
                picked = picked + mm(
                    ns[:, 256 * tile : 256 * tile + 256], selector(lo, hi, tile, iota)
                )
            picked = picked.astype(bf16)
            sendb[2 * pair] = picked[:, :HALO]
            sendb[2 * pair + 1] = picked[:, HALO:]
            col_p[256 * pair : 256 * pair + 256, :] = columns_of(lo, hi)

        ghost[4 + s] = jnp.zeros((D, HALO), bf16)
        gback[4 + s] = jnp.zeros((D, HALO), bf16)

        forward = []
        backward = []
        if comm:
            pl.semaphore_wait(barrier, len(peers))
            for number, (o, r) in enumerate(halo_pairs):
                t = lax.rem(s + r, 4)
                forward.append(
                    pltpu.make_async_remote_copy(
                        src_ref=sendb.at[o * 4 + t],
                        dst_ref=ghost.at[o * 4 + s],
                        send_sem=sem_fs.at[number],
                        recv_sem=sem_fr.at[o * 4 + s],
                        device_id=row_peer(o - 1, r),
                        device_id_type=MESH,
                    )
                )
            for copy in forward:
                copy.start()

        for k in (2, 3, 1, 7, 8, 9, 10, 11, 12, 13, 14, 15):
            loads[k].wait()
        vec[0] = column_of(b1[...])
        vec[1] = column_of(eg[...])
        vec[2] = column_of(esh[...])
        vec[3] = column_of(nb1[...])
        vec[4] = column_of(ng[...])
        w1[...] = w1t[...].astype(f32).T.astype(bf16)
        w2t[...] = w2[...].astype(f32).T.astype(bf16)
        nw1[...] = nw1t[...].astype(f32).T.astype(bf16)
        nw2t[...] = nw2[...].astype(f32).T.astype(bf16)
        sums[...] = jnp.zeros_like(sums)
        stk[128:192, :] = es[...]
        nin[0:64, :] = ns[...]

        def gather_own(i, carry):
            at = pl.ds(pl.multiple_of(i * BLK, BLK), BLK) if not isinstance(i, int) else slice(i * BLK, i * BLK + BLK)
            for index, begin, cols in ((snd, 0, col_s), (rcv, 64, col_r)):
                lo, hi = split_index(index[:, at])
                total = jnp.zeros((D, BLK), f32)
                for tile in range(4):
                    total = total + mm(
                        ns[:, 256 * tile : 256 * tile + 256], selector(lo, hi, tile, iota2)
                    )
                stk[begin : begin + 64, at] = total.astype(bf16)
                cols[at, :] = columns_of(lo, hi)
            return carry

        for i in range(NF // BLK):
            gather_own(i, 0)

        if comm:
            for o, r in halo_pairs:
                t = lax.rem(s + r, 4)
                pltpu.make_async_remote_copy(
                    src_ref=sendb.at[o * 4 + t],
                    dst_ref=ghost.at[o * 4 + t],
                    send_sem=sem_fs.at[0],
                    recv_sem=sem_fr.at[o * 4 + t],
                    device_id=row_peer(o - 1, r),
                    device_id_type=MESH,
                ).wait_recv()

        def forward_faces(i, carry):
            at = pl.ds(pl.multiple_of(i * BLK, BLK), BLK) if not isinstance(i, int) else slice(i * BLK, i * BLK + BLK)
            lo, hi = split_index(snd[:, at])
            total = stk[0:64, at].astype(f32)
            for pair in range(NB // 2):
                table = jnp.concatenate([ghost[2 * pair], ghost[2 * pair + 1]], axis=1)
                total = total + mm(table, selector(lo, hi, 4 + pair, iota2))
            stk[0:64, at] = total.astype(bf16)
            linear = mm(w1t[...], stk[0:192, at]) + wide(vec[0], BLK)
            gate = logistic(linear)
            active = (linear * gate).astype(bf16)
            stk[192:256, at] = active
            slope[:, at] = gate * (1.0 + linear * (1.0 - gate))
            scaled, spread = standardize(mm(w2t[...], active))
            scl[:, at] = scaled
            spr[:, at] = spread
            msg[:, at] = (scaled * wide(vec[1], BLK) + wide(vec[2], BLK)).astype(bf16)
            return carry

        for i in range(NF // BLK):
            forward_faces(i, 0)

        acc[:, 0:NC] = jnp.zeros((D, NC), f32)

        def sum_messages(i, carry):
            at = pl.ds(pl.multiple_of(i * BLK, BLK), BLK) if not isinstance(i, int) else slice(i * BLK, i * BLK + BLK)
            lo, hi = col_r[at, 0:128], col_r[at, 128:256]
            part = msg[:, at]
            for tile in range(4):
                where = slice(256 * tile, 256 * tile + 256)
                acc[:, where] += mm(part, selector_t(lo, hi, tile, iotas))
            return carry

        for i in range(NF // BLK):
            sum_messages(i, 0)

        loads[5].wait()
        loads[6].wait()
        def cells(i, carry):
            at = pl.ds(pl.multiple_of(i * BLK, BLK), BLK) if not isinstance(i, int) else slice(i * BLK, i * BLK + BLK)
            nin[64:128, at] = acc[:, at].astype(bf16)
            linear = mm(nw1t[...], nin[0:128, at]) + wide(vec[3], BLK)
            gate = logistic(linear)
            active = (linear * gate).astype(bf16)
            nin[128:192, at] = active
            scaled, spread = standardize(mm(nw2t[...], active))
            upstream = nct[:, at].astype(f32)
            sums[4] += fold_lanes(upstream * scaled)
            sums[5] += fold_lanes(upstream)
            delta = normalize_back(upstream, scaled, spread, wide(vec[4], BLK)).astype(bf16)
            nh2[0:64, at] = delta
            hidden = mm(nw2[...], delta) * (gate * (1.0 + linear * (1.0 - gate)))
            sums[3] += fold_lanes(hidden)
            hidden = hidden.astype(bf16)
            nh2[64:128, at] = hidden
            back = mm(nw1[...], hidden)
            own[:, at] = back[0:64] + upstream
            nbr[:, at] = back[64:128].astype(bf16)
            return carry

        for i in range(NC // BLK):
            cells(i, 0)

        def backward_faces(i, carry):
            at = pl.ds(pl.multiple_of(i * BLK, BLK), BLK) if not isinstance(i, int) else slice(i * BLK, i * BLK + BLK)
            lo, hi = split_index(rcv[:, at])
            cotangent = ect[:, at].astype(f32)
            upstream = cotangent
            for tile in range(4):
                upstream = upstream + mm(
                    nbr[:, 256 * tile : 256 * tile + 256], selector(lo, hi, tile, iota2)
                )
            scaled = scl[:, at]
            sums[1] += fold_lanes(upstream * scaled)
            sums[2] += fold_lanes(upstream)
            delta = normalize_back(upstream, scaled, spr[:, at], wide(vec[1], BLK)).astype(bf16)
            ehd[64:128, at] = delta
            hidden = mm(w2[...], delta) * slope[:, at]
            sums[0] += fold_lanes(hidden)
            hidden = hidden.astype(bf16)
            ehd[0:64, at] = hidden
            dedges[:, at] = (cotangent + mm(w1[128:192, :], hidden)).astype(bf16)
            return carry

        for i in range(NF // BLK):
            backward_faces(i, 0)

        edge_part = mm_last(stk[...], ehd[...])
        node_part = mm_last(nin[...], nh2[...])
        lane64 = lax.broadcasted_iota(jnp.int32, (64, 128), 1)
        vectors = jnp.zeros((64, 128), f32)
        for number in range(6):
            vectors = jnp.where(
                lane64 == 64 + number, jnp.sum(sums[number], axis=1, keepdims=True), vectors
            )
        grads[0:64] = jnp.where(lane64 < 64, edge_part[0:64], node_part[0:64])
        grads[64:128] = jnp.where(lane64 < 64, edge_part[64:128], node_part[64:128])
        grads[128:192] = jnp.where(lane64 < 64, edge_part[128:192], vectors)
        grads[192:256] = jnp.where(lane64 < 64, node_part[128:192], edge_part[192:256])

        first = []
        if comm:
            for j in range(1, 8):
                other, peer = a_peer(j)
                first.append(
                    pltpu.make_async_remote_copy(
                        src_ref=grads.at[pl.ds(pl.multiple_of(other * 32, 32), 32), :],
                        dst_ref=rs_buf.at[a],
                        send_sem=sem_rs.at[j],
                        recv_sem=sem_rr.at[a],
                        device_id=peer,
                        device_id_type=MESH,
                    )
                )
            for copy in first:
                copy.start()

        acc[...] = jnp.zeros_like(acc)

        def sum_ghosts(i, carry):
            at = pl.ds(pl.multiple_of(i * BLK, BLK), BLK) if not isinstance(i, int) else slice(i * BLK, i * BLK + BLK)
            lo, hi = col_s[at, 0:128], col_s[at, 128:256]
            part = ehd[0:64, at]
            for tile in range(6):
                where = slice(256 * tile, 256 * tile + 256)
                acc[:, where] += mm(part, selector_t(lo, hi, 4 + tile, iotas))
            return carry

        for i in range(NF // BLK):
            sum_ghosts(i, 0)
        for pair in range(NB // 2):
            block = mm(
                w1[0:64, :], acc[:, 256 * pair : 256 * pair + 256].astype(bf16)
            ).astype(bf16)
            gsend[2 * pair] = block[:, :HALO]
            gsend[2 * pair + 1] = block[:, HALO:]
        if comm:
            for number, (o, r) in enumerate(halo_pairs):
                t = lax.rem(s + r, 4)
                backward.append(
                    pltpu.make_async_remote_copy(
                        src_ref=gsend.at[o * 4 + t],
                        dst_ref=gback.at[o * 4 + s],
                        send_sem=sem_bs.at[number],
                        recv_sem=sem_br.at[o * 4 + s],
                        device_id=row_peer(1 - o, r),
                        device_id_type=MESH,
                    )
                )
            for copy in backward:
                copy.start()

        second = []
        if comm:
            total = grads[pl.ds(pl.multiple_of(a * 32, 32), 32), :]
            for j in range(1, 8):
                other, peer = a_peer(j)
                pltpu.make_async_remote_copy(
                    src_ref=rs_buf.at[other],
                    dst_ref=rs_buf.at[other],
                    send_sem=sem_rs.at[j],
                    recv_sem=sem_rr.at[other],
                    device_id=peer,
                    device_id_type=MESH,
                ).wait_recv()
                total = total + rs_buf[other]
            ex_buf[b] = total
            for j in range(1, 16):
                other, peer = b_peer(j)
                second.append(
                    pltpu.make_async_remote_copy(
                        src_ref=ex_buf.at[b],
                        dst_ref=ex_buf.at[b],
                        send_sem=sem_es.at[j],
                        recv_sem=sem_er.at[b],
                        device_id=peer,
                        device_id_type=MESH,
                    )
                )
            for copy in second:
                copy.start()

        acc[:, 0:NC] = jnp.zeros((D, NC), f32)
        gt[...] = jnp.zeros_like(gt)

        def sum_own(i, carry):
            at = pl.ds(pl.multiple_of(i * BLK, BLK), BLK) if not isinstance(i, int) else slice(i * BLK, i * BLK + BLK)
            part = ehd[0:64, at]
            for cols, total in ((col_s, acc), (col_r, gt)):
                lo, hi = cols[at, 0:128], cols[at, 128:256]
                for tile in range(4):
                    where = slice(256 * tile, 256 * tile + 256)
                    total[:, where] += mm(part, selector_t(lo, hi, tile, iotas))
            return carry

        for i in range(NF // BLK):
            sum_own(i, 0)
        own[...] += mm(w1[0:64, :], acc[:, 0:NC].astype(bf16)) + mm(
            w1[64:128, :], gt[...].astype(bf16)
        )

        third = []
        if comm:
            for j in range(1, 16):
                other, peer = b_peer(j)
                pltpu.make_async_remote_copy(
                    src_ref=ex_buf.at[other],
                    dst_ref=ex_buf.at[other],
                    send_sem=sem_es.at[j],
                    recv_sem=sem_er.at[other],
                    device_id=peer,
                    device_id_type=MESH,
                ).wait_recv()
            total = ex_buf[0]
            for j in range(1, 16):
                total = total + ex_buf[j]
            ag_buf[a] = total
            for j in range(1, 8):
                other, peer = a_peer(j)
                third.append(
                    pltpu.make_async_remote_copy(
                        src_ref=ag_buf.at[a],
                        dst_ref=ag_buf.at[a],
                        send_sem=sem_as.at[j],
                        recv_sem=sem_ar.at[a],
                        device_id=peer,
                        device_id_type=MESH,
                    )
                )
            for copy in third:
                copy.start()

            for o, r in halo_pairs:
                t = lax.rem(s + r, 4)
                pltpu.make_async_remote_copy(
                    src_ref=gsend.at[o * 4 + t],
                    dst_ref=gback.at[o * 4 + t],
                    send_sem=sem_bs.at[0],
                    recv_sem=sem_br.at[o * 4 + t],
                    device_id=row_peer(1 - o, r),
                    device_id_type=MESH,
                ).wait_recv()

        returned = jnp.concatenate([gback[k] for k in range(NB)], axis=1)
        for tile in range(4):
            where = slice(256 * tile, 256 * tile + 256)
            total = own[:, where]
            for pair in range(NB // 2):
                at = slice(256 * pair, 256 * pair + 256)
                total = total + mm(
                    returned[:, at],
                    selector_t(col_p[at, 0:128], col_p[at, 128:256], tile, iotas),
                )
            dstate[:, where] = total.astype(bf16)

        if comm:
            for j in range(1, 8):
                other, peer = a_peer(j)
                pltpu.make_async_remote_copy(
                    src_ref=ag_buf.at[other],
                    dst_ref=ag_buf.at[other],
                    send_sem=sem_as.at[j],
                    recv_sem=sem_ar.at[other],
                    device_id=peer,
                    device_id_type=MESH,
                ).wait_recv()
            for j in range(8):
                packed[32 * j : 32 * j + 32] = ag_buf[j]
        else:
            packed[...] = grads[...]
        for copy in forward + backward + first + second + third:
            copy.wait_send()

    return kernel


def finish(
    dstate, dedges, packed, out_state, out_edges, *refs
):
    results, refs = refs[:10], refs[10:]
    staged, sems = refs[:10], refs[10]
    o_w1, o_b1, o_w2, o_eg, o_es, o_nw1, o_nb1, o_nw2, o_ng, o_ns = staged
    stores = [
        pltpu.make_async_copy(dedges, out_edges, sems.at[10]),
        pltpu.make_async_copy(dstate, out_state, sems.at[11]),
    ]
    for copy in stores:
        copy.start()
    whole = packed[...] * FACTOR
    turned = jnp.concatenate([whole[0:128].T, whole[128:256].T], axis=1)
    o_w1[...] = turned[0:64, 0:192]
    o_nw1[...] = turned[64:128, 0:128]
    o_nw2[...] = whole[192:256, 0:64]
    o_w2[...] = pltpu.roll(whole[192:256], 64, 1)[:, 0:64]
    rows = turned[64:128, 128:192]
    for k, ref in enumerate((o_b1, o_eg, o_es, o_nb1, o_ng, o_ns)):
        ref[...] = rows[k : k + 1, :]
    for k in range(10):
        copy = pltpu.make_async_copy(staged[k], results[k], sems.at[k])
        copy.start()
        stores.append(copy)
    for copy in stores:
        copy.wait()


def call(comm, *args):
    shapes = [
        ((D, NC), bf16),
        ((D, NF), bf16),
        ((64, 192), f32),
        ((1, 64), f32),
        ((64, 64), f32),
        ((1, 64), f32),
        ((1, 64), f32),
        ((64, 128), f32),
        ((1, 64), f32),
        ((64, 64), f32),
        ((1, 64), f32),
        ((1, 64), f32),
    ]
    dma = pltpu.SemaphoreType.DMA
    scratch = [pltpu.VMEM(arg.shape, arg.dtype) for arg in args]
    scratch += [
        pltpu.VMEM((256, NF), bf16),
        pltpu.VMEM((D, NF), f32),
        pltpu.VMEM((D, NF), f32),
        pltpu.VMEM((1, NF), f32),
        pltpu.VMEM((D, NF), bf16),
        pltpu.VMEM((128, NF), bf16),
        pltpu.VMEM((NF, 256), bf16),
        pltpu.VMEM((NF, 256), bf16),
        pltpu.VMEM((NB * HALO, 256), bf16),
        pltpu.VMEM((NB, D, HALO), bf16),
        pltpu.VMEM((NB, D, HALO), bf16),
        pltpu.VMEM((NB, D, HALO), bf16),
        pltpu.VMEM((NB, D, HALO), bf16),
        pltpu.VMEM((192, NC), bf16),
        pltpu.VMEM((128, NC), bf16),
        pltpu.VMEM((D, NC), bf16),
        pltpu.VMEM((D, NC), f32),
        pltpu.VMEM((D, NB * HALO), f32),
        pltpu.VMEM((D, NC), f32),
        pltpu.VMEM((D, HALO), bf16),
        pltpu.VMEM((5, D, 128), f32),
        pltpu.VMEM((6, D, 128), f32),
        pltpu.VMEM((256, 128), f32),
        pltpu.VMEM((8, 32, 128), f32),
        pltpu.VMEM((16, 32, 128), f32),
        pltpu.VMEM((8, 32, 128), f32),
        pltpu.VMEM((192, 64), bf16),
        pltpu.VMEM((64, 64), bf16),
        pltpu.VMEM((128, 64), bf16),
        pltpu.VMEM((64, 64), bf16),
        dma((12,)), dma((12,)), dma((12,)), dma((12,)),
        dma((8,)), dma((8,)), dma((16,)), dma((16,)), dma((8,)), dma((8,)),
        dma((16,)),
    ]
    anywhere = pl.BlockSpec(memory_space=pltpu.HBM)
    params = dict(vmem_limit_bytes=36 * 1024 * 1024)
    if comm:
        params.update(collective_id=0, has_side_effects=True)
    vmem = pl.BlockSpec(memory_space=pltpu.VMEM)
    middle = pl.pallas_call(
        make_kernel(comm),
        out_shape=[
            jax.ShapeDtypeStruct(shape, kind) for shape, kind in shapes[:2] + [((256, 128), f32)]
        ],
        in_specs=[anywhere] * 16,
        out_specs=[vmem] * 3,
        scratch_shapes=scratch,
        compiler_params=pltpu.CompilerParams(**params),
        name="layer",
    )(*[pltpu.with_memory_space_constraint(arg, pltpu.HBM) for arg in args])
    return pl.pallas_call(
        finish,
        out_shape=[jax.ShapeDtypeStruct(shape, kind) for shape, kind in shapes],
        in_specs=[vmem] * 3,
        out_specs=[anywhere] * 12,
        scratch_shapes=[pltpu.VMEM(shape, kind) for shape, kind in shapes[2:]] + [dma((12,))],
        compiler_params=pltpu.CompilerParams(vmem_limit_bytes=8 * 1024 * 1024),
        name="finish",
    )(*middle)


def on_device(comm, node_state, edge_state, senders, receivers, send_index, node_cotangent, edge_cotangent,
              edge_first, edge_bias, edge_second, edge_gain, edge_shift, node_first, node_bias, node_second, node_gain):
    line = lambda v: v.reshape(1, -1)
    outs = call(
        comm, node_state, edge_state, line(senders), line(receivers), line(send_index),
        node_cotangent, edge_cotangent, edge_first.T, line(edge_bias), edge_second, line(edge_gain),
        line(edge_shift), node_first.T, line(node_bias), node_second, line(node_gain),
    )
    outs = [v.reshape(-1) if v.shape[0] == 1 else v for v in outs]
    outs[2] = outs[2].T
    outs[7] = outs[7].T
    return tuple(outs)


def solution(mesh):
    split = Mesh(mesh.devices.reshape(4, 4, 2, 4), AXES)
    every = P(None, AXES)
    in_specs = (every, every, P(AXES), P(AXES), P(AXES, None, None), every, every) + (P(),) * 9
    out_specs = (every, every) + (P(),) * 10
    return jax.shard_map(
        lambda *args: on_device(True, *args), mesh=split, in_specs=in_specs, out_specs=out_specs,
        check_vma=False,
    )
```

```python
import math

import jax
import jax.numpy as jnp
from jax import lax
from jax.experimental import pallas as pl
from jax.experimental.pallas import tpu as pltpu
from jax.sharding import Mesh
from jax.sharding import PartitionSpec as P

AXES = ("z", "y", "core", "sub")
MESH = pl.DeviceIdType.MESH
EPSILON = 1e-05
D = 64
NF = 3072
NC = 1024
NB = 12
HALO = 128
BLK = 512
bf16 = jnp.bfloat16
f32 = jnp.float32
i16 = jnp.int16
FACTOR = 1.0 / math.sqrt(393216)


def mm(a, b):
    return jnp.dot(a, b, preferred_element_type=f32)


def mm_last(a, b):
    return lax.dot_general(a, b, (((1,), (1,)), ((), ())), preferred_element_type=f32)


def rows_of(index):
    return jnp.broadcast_to(index, (16, index.shape[1])).astype(i16)


def selector(rows, tile):
    width = rows.shape[1]
    iota = lax.broadcasted_iota(jnp.int32, (256, 128), 0).astype(i16)
    iota = jnp.concatenate([iota] * (width // 128), axis=1)
    key = jnp.concatenate([rows - i16(256 * tile)] * 16, axis=0)
    return jnp.where(iota == key, bf16(1), bf16(0))


def columns_of(index):
    width = index.shape[1]
    sub = lax.broadcasted_iota(jnp.int32, (8, width), 0)
    low, high = index & 255, index >> 8
    parts = jnp.where(sub == 0, low, jnp.where(sub == 1, high, 0)).astype(f32)
    sub = lax.broadcasted_iota(jnp.int32, (8, 128), 0)
    scale = jnp.where(sub == 0, 1.0, jnp.where(sub == 1, 256.0, 0.0))
    out = lax.dot_general(parts, scale, (((0,), (0,)), ((), ())), preferred_element_type=f32)
    return out.astype(jnp.int32).astype(i16)


def selector_t(column, tile):
    lane = lax.broadcasted_iota(jnp.int32, (16, 128), 1).astype(i16)
    halves = []
    for half in range(2):
        key = jnp.concatenate([lane + i16(256 * tile + 128 * half)] * (column.shape[0] // 16), axis=0)
        halves.append(jnp.where(column == key, bf16(1), bf16(0)))
    return jnp.concatenate(halves, axis=1)


def staged(stages, count):
    for step in range(count + len(stages) - 1):
        for depth, stage in enumerate(stages):
            if 0 <= step - depth < count:
                stage(step - depth)


def block_at(i):
    return slice(i * BLK, i * BLK + BLK)


def column_of(row):
    sub = lax.broadcasted_iota(jnp.int32, (D, D), 0)
    lane = lax.broadcasted_iota(jnp.int32, (D, D), 1)
    col = jnp.sum(jnp.where(sub == lane, row, 0.0), axis=1, keepdims=True)
    return jnp.broadcast_to(col, (D, 128))


def wide(col, width):
    return jnp.concatenate([col] * (width // 128), axis=1)


def fold_lanes(values):
    total = values[:, 0:128]
    for begin in range(128, values.shape[1], 128):
        total = total + values[:, begin : begin + 128]
    return total


def mean_rows(values):
    return jnp.sum(values, axis=0, keepdims=True) * (1.0 / D)


def logistic(values):
    return 0.5 * jnp.tanh(0.5 * values) + 0.5


def standardize(values):
    centered = values - mean_rows(values)
    spread = lax.rsqrt(mean_rows(centered * centered) + EPSILON)
    return centered * spread, spread


def normalize_back(upstream, scaled, spread, gain):
    weighted = upstream * gain
    return spread * (weighted - mean_rows(weighted) - scaled * mean_rows(weighted * scaled))


def make_kernel(comm):
    def kernel(
        *refs
    ):
        given, refs = refs[:16], refs[16:]
        (dstate, dedges, packed), refs = refs[:3], refs[3:]
        held, refs = refs[:16], refs[16:]
        (
            stk, slope, scl, ups, spr, msg, ehd, col_s, col_r, col_p,
            sendb, ghost, gsend, gback, nin, nh2, nbr, own, acc, gac, gt,
            vec, sums, grads, shared, rs_buf, ex_buf, ag_buf, w1, w2t, nw1, nw2t,
            sem_fs, sem_fr, sem_bs, sem_br, sem_rs, sem_rr, sem_es, sem_er, sem_as, sem_ar,
            sem_in,
        ) = refs
        ns, es, snd, rcv, six, nct, ect, w1t, b1, w2, eg, esh, nw1t, nb1, nw2, ng = held
        loads = [
            pltpu.make_async_copy(given[k], held[k], sem_in.at[k]) for k in range(16)
        ]
        for k in (4, 0, 2, 3, 1, 7, 8, 9, 10, 11, 12, 13, 14, 15, 5, 6):
            loads[k].start()
        if comm:
            z = lax.axis_index("z")
            y = lax.axis_index("y")
            core = lax.axis_index("core")
            s = lax.axis_index("sub")
            d = z * 8 + y * 2 + core
            a = z * 2 + core
            b = y * 4 + s

            def row_peer(step, t):
                dd = lax.rem(d + (step + 32), 32)
                return lax.div(dd, 8), lax.rem(lax.div(dd, 2), 4), lax.rem(dd, 2), t

            def a_peer(j):
                other = lax.rem(a + j, 8)
                return other, (lax.div(other, 2), y, lax.rem(other, 2), s)

            def b_peer(j):
                other = lax.rem(b + j, 16)
                return other, (z, lax.div(other, 4), core, lax.rem(other, 4))

            halo_pairs = [(o, r) for o in range(3) for r in range(4) if not (o == 1 and r == 0)]
            barrier = pltpu.get_barrier_semaphore()
            peers = [row_peer(o - 1, lax.rem(s + r, 4)) for o, r in halo_pairs]
            peers += [a_peer(j)[1] for j in range(1, 8)] + [b_peer(j)[1] for j in range(1, 16)]
            for peer in peers:
                pl.semaphore_signal(barrier, inc=1, device_id=peer, device_id_type=MESH)
        else:
            s = 0

        def waits(copies):
            for condition, copy in copies:
                if condition is None:
                    copy.wait_send()
                else:
                    pl.when(condition)(copy.wait_send)

        def send_block(k, source, target, sems, turn):
            o, t = k // 4, k % 4
            copy = pltpu.make_async_remote_copy(
                src_ref=source.at[k],
                dst_ref=target.at[o * 4 + s],
                send_sem=sems[0].at[k],
                recv_sem=sems[1].at[o * 4 + s],
                device_id=row_peer(turn * (o - 1), t),
                device_id_type=MESH,
            )
            condition = s != t if o == 1 else None
            if condition is None:
                copy.start()
            else:
                pl.when(condition)(copy.start)
            return condition, copy

        def receive_blocks(source, target, sems):
            for o, r in halo_pairs:
                slot = o * 4 + lax.rem(s + r, 4)
                pltpu.make_async_remote_copy(
                    src_ref=source.at[slot],
                    dst_ref=target.at[slot],
                    send_sem=sems[0].at[0],
                    recv_sem=sems[1].at[slot],
                    device_id=row_peer(o - 1, lax.rem(s + r, 4)),
                    device_id_type=MESH,
                ).wait_recv()

        loads[4].wait()
        loads[0].wait()
        forward = []
        for place, pair in enumerate((0, 1, 4, 5, 2, 3)):
            rows = rows_of(six[:, 256 * pair : 256 * pair + 256])
            picked = jnp.zeros((D, 256), f32)
            for tile in range(4):
                picked = picked + mm(ns[:, 256 * tile : 256 * tile + 256], selector(rows, tile))
            picked = picked.astype(bf16)
            sendb[2 * pair] = picked[:, :HALO]
            sendb[2 * pair + 1] = picked[:, HALO:]
            if comm:
                if place == 0:
                    pl.semaphore_wait(barrier, len(peers))
                for k in (2 * pair, 2 * pair + 1):
                    forward.append(send_block(k, sendb, ghost, (sem_fs, sem_fr), 1))

        ghost[4 + s] = jnp.zeros((D, HALO), bf16)
        gback[4 + s] = jnp.zeros((D, HALO), bf16)
        for k in (2, 3, 1, 7, 8, 9, 10, 11, 12, 13, 14, 15):
            loads[k].wait()
        vec[0] = column_of(b1[...])
        vec[1] = column_of(eg[...])
        vec[2] = column_of(esh[...])
        vec[3] = column_of(nb1[...])
        vec[4] = column_of(ng[...])
        w1[...] = w1t[...].astype(f32).T.astype(bf16)
        w2t[...] = w2[...].astype(f32).T.astype(bf16)
        nw1[...] = nw1t[...].astype(f32).T.astype(bf16)
        nw2t[...] = nw2[...].astype(f32).T.astype(bf16)
        sums[...] = jnp.zeros_like(sums)
        stk[128:192, :] = es[...]
        nin[0:64, :] = ns[...]

        def gather_own(i):
            at = block_at(i)
            for index, begin in ((snd, 0), (rcv, 64)):
                rows = rows_of(index[:, at])
                total = jnp.zeros((D, BLK), f32)
                for tile in range(4):
                    total = total + mm(ns[:, 256 * tile : 256 * tile + 256], selector(rows, tile))
                stk[begin : begin + 64, at] = total.astype(bf16)
            col_s[at, :] = columns_of(snd[:, at])
            col_r[at, :] = columns_of(rcv[:, at])

        staged([gather_own], NF // BLK)
        for pair in range(NB // 2):
            at = slice(256 * pair, 256 * pair + 256)
            col_p[at, :] = columns_of(six[:, at])

        if comm:
            receive_blocks(sendb, ghost, (sem_fs, sem_fr))

        def gather_ghosts(i):
            at = block_at(i)
            rows = rows_of(snd[:, at])
            total = stk[0:64, at].astype(f32)
            for pair in range(NB // 2):
                table = jnp.concatenate([ghost[2 * pair], ghost[2 * pair + 1]], axis=1)
                total = total + mm(table, selector(rows, 4 + pair))
            stk[0:64, at] = total.astype(bf16)

        def forward_faces(i):
            at = block_at(i)
            linear = mm(w1t[...], stk[0:192, at]) + wide(vec[0], BLK)
            gate = logistic(linear)
            activated = linear * gate
            active = activated.astype(bf16)
            stk[192:256, at] = active
            slope[:, at] = gate + activated * (1.0 - gate)
            scaled, spread = standardize(mm(w2t[...], active))
            scl[:, at] = scaled
            spr[:, at] = spread
            msg[:, at] = (scaled * wide(vec[1], BLK) + wide(vec[2], BLK)).astype(bf16)

        def scatter(i, part, column, total, tiles, first):
            for tile in tiles:
                where = slice(256 * (tile - tiles[0]), 256 * (tile - tiles[0]) + 256)
                added = mm(part, selector_t(column, tile))
                total[:, where] = added if first else total[:, where] + added

        def sum_messages(i):
            at = block_at(i)
            scatter(i, msg[:, at], col_r[at, :], acc, range(4), i == 0)

        staged([gather_ghosts, forward_faces, sum_messages], NF // BLK)

        loads[5].wait()
        loads[6].wait()
        def cells(i):
            at = block_at(i)
            nin[64:128, at] = acc[:, at].astype(bf16)
            linear = mm(nw1t[...], nin[0:128, at]) + wide(vec[3], BLK)
            gate = logistic(linear)
            activated = linear * gate
            active = activated.astype(bf16)
            nin[128:192, at] = active
            scaled, spread = standardize(mm(nw2t[...], active))
            upstream = nct[:, at].astype(f32)
            sums[4] += fold_lanes(upstream * scaled)
            sums[5] += fold_lanes(upstream)
            delta = normalize_back(upstream, scaled, spread, wide(vec[4], BLK)).astype(bf16)
            nh2[0:64, at] = delta
            hidden = mm(nw2[...], delta) * (gate + activated * (1.0 - gate))
            sums[3] += fold_lanes(hidden)
            hidden = hidden.astype(bf16)
            nh2[64:128, at] = hidden
            back = mm(nw1[...], hidden)
            own[:, at] = back[0:64] + upstream
            nbr[:, at] = back[64:128].astype(bf16)

        staged([cells], NC // BLK)

        def gather_back(i):
            at = block_at(i)
            rows = rows_of(rcv[:, at])
            upstream = ect[:, at].astype(f32)
            for tile in range(4):
                upstream = upstream + mm(
                    nbr[:, 256 * tile : 256 * tile + 256], selector(rows, tile)
                )
            ups[:, at] = upstream

        def backward_faces(i):
            at = block_at(i)
            upstream = ups[:, at]
            scaled = scl[:, at]
            sums[1] += fold_lanes(upstream * scaled)
            sums[2] += fold_lanes(upstream)
            delta = normalize_back(upstream, scaled, spr[:, at], wide(vec[1], BLK)).astype(bf16)
            ehd[64:128, at] = delta
            hidden = mm(w2[...], delta) * slope[:, at]
            sums[0] += fold_lanes(hidden)
            ehd[0:64, at] = hidden.astype(bf16)

        def sum_ghosts(i):
            at = block_at(i)
            scatter(i, ehd[0:64, at], col_s[at, :], gac, range(4, 10), i == 0)

        staged([gather_back, backward_faces, sum_ghosts], NF // BLK)

        edge_part = mm_last(stk[...], ehd[...])
        node_part = mm_last(nin[...], nh2[...])
        lane64 = lax.broadcasted_iota(jnp.int32, (64, 128), 1)
        vectors = jnp.zeros((64, 128), f32)
        for number in range(6):
            vectors = jnp.where(
                lane64 == 64 + number, jnp.sum(sums[number], axis=1, keepdims=True), vectors
            )
        high = vectors.astype(bf16).astype(f32)
        vectors = high + pltpu.roll(vectors - high, 6, 1)
        grads[0:64] = jnp.where(lane64 < 64, edge_part[0:64], node_part[0:64])
        grads[64:128] = jnp.where(lane64 < 64, edge_part[64:128], node_part[64:128])
        grads[128:192] = jnp.where(lane64 < 64, edge_part[128:192], vectors)
        grads[192:256] = jnp.where(lane64 < 64, node_part[128:192], edge_part[192:256])

        first = []
        if comm:
            shared[...] = grads[...].astype(bf16)
            for j in range(1, 8):
                other, peer = a_peer(j)
                first.append(
                    pltpu.make_async_remote_copy(
                        src_ref=shared.at[pl.ds(pl.multiple_of(other * 32, 32), 32), :],
                        dst_ref=rs_buf.at[a],
                        send_sem=sem_rs.at[j],
                        recv_sem=sem_rr.at[a],
                        device_id=peer,
                        device_id_type=MESH,
                    )
                )
            for copy in first:
                copy.start()

        backward = []
        for pair in (0, 1, 4, 5, 2, 3):
            block = mm(w1[0:64, :], gac[:, 256 * pair : 256 * pair + 256].astype(bf16)).astype(bf16)
            gsend[2 * pair] = block[:, :HALO]
            gsend[2 * pair + 1] = block[:, HALO:]
            if comm:
                for k in (2 * pair, 2 * pair + 1):
                    backward.append(send_block(k, gsend, gback, (sem_bs, sem_br), -1))

        for i in range(NF // BLK):
            at = block_at(i)
            dedges[:, at] = (ect[:, at].astype(f32) + mm(w1[128:192, :], ehd[0:64, at])).astype(bf16)

        def split_vectors(total):
            lane = lax.broadcasted_iota(jnp.int32, (32, 128), 1)
            whole = total + pltpu.roll(total, 122, 1)
            high = whole.astype(bf16).astype(f32)
            parts = jnp.where(lane < 70, high, pltpu.roll(whole - high, 6, 1))
            return jnp.where(((a == 4) | (a == 5)) & (lane >= 64) & (lane < 76), parts, total)

        second = []
        if comm:
            total = grads[pl.ds(pl.multiple_of(a * 32, 32), 32), :]
            for j in range(1, 8):
                other, peer = a_peer(j)
                pltpu.make_async_remote_copy(
                    src_ref=rs_buf.at[other],
                    dst_ref=rs_buf.at[other],
                    send_sem=sem_rs.at[j],
                    recv_sem=sem_rr.at[other],
                    device_id=peer,
                    device_id_type=MESH,
                ).wait_recv()
                total = total + rs_buf[other].astype(f32)
            ex_buf[b] = split_vectors(total).astype(bf16)
            for j in range(1, 16):
                other, peer = b_peer(j)
                second.append(
                    pltpu.make_async_remote_copy(
                        src_ref=ex_buf.at[b],
                        dst_ref=ex_buf.at[b],
                        send_sem=sem_es.at[j],
                        recv_sem=sem_er.at[b],
                        device_id=peer,
                        device_id_type=MESH,
                    )
                )
            for copy in second:
                copy.start()

        def sum_own(i):
            at = block_at(i)
            scatter(i, ehd[0:64, at], col_s[at, :], acc, range(4), i == 0)
            scatter(i, ehd[0:64, at], col_r[at, :], gt, range(4), i == 0)

        staged([sum_own], NF // BLK)
        own[...] += mm(w1[0:64, :], acc[...].astype(bf16)) + mm(w1[64:128, :], gt[...].astype(bf16))

        third = []
        if comm:
            for j in range(1, 16):
                other, peer = b_peer(j)
                pltpu.make_async_remote_copy(
                    src_ref=ex_buf.at[other],
                    dst_ref=ex_buf.at[other],
                    send_sem=sem_es.at[j],
                    recv_sem=sem_er.at[other],
                    device_id=peer,
                    device_id_type=MESH,
                ).wait_recv()
            total = ex_buf[0].astype(f32)
            for j in range(1, 16):
                total = total + ex_buf[j].astype(f32)
            ag_buf[a] = split_vectors(total).astype(bf16)
            for j in range(1, 8):
                other, peer = a_peer(j)
                third.append(
                    pltpu.make_async_remote_copy(
                        src_ref=ag_buf.at[a],
                        dst_ref=ag_buf.at[a],
                        send_sem=sem_as.at[j],
                        recv_sem=sem_ar.at[a],
                        device_id=peer,
                        device_id_type=MESH,
                    )
                )
            for copy in third:
                copy.start()

            receive_blocks(gsend, gback, (sem_bs, sem_br))

        returned = jnp.concatenate([gback[k] for k in range(NB)], axis=1)
        for tile in range(4):
            where = slice(256 * tile, 256 * tile + 256)
            total = own[:, where]
            for pair in range(NB // 2):
                at = slice(256 * pair, 256 * pair + 256)
                total = total + mm(returned[:, at], selector_t(col_p[at, :], tile))
            dstate[:, where] = total.astype(bf16)

        if comm:
            for j in range(1, 8):
                other, peer = a_peer(j)
                pltpu.make_async_remote_copy(
                    src_ref=ag_buf.at[other],
                    dst_ref=ag_buf.at[other],
                    send_sem=sem_as.at[j],
                    recv_sem=sem_ar.at[other],
                    device_id=peer,
                    device_id_type=MESH,
                ).wait_recv()
            for j in range(8):
                packed[32 * j : 32 * j + 32] = ag_buf[j].astype(f32)
        else:
            packed[...] = grads[...]
        waits(forward + backward)
        for copy in first + second + third:
            copy.wait_send()

    return kernel


def finish(
    dstate, dedges, packed, out_state, out_edges, *refs
):
    results, refs = refs[:10], refs[10:]
    staged, sems = refs[:10], refs[10]
    o_w1, o_b1, o_w2, o_eg, o_es, o_nw1, o_nb1, o_nw2, o_ng, o_ns = staged
    stores = [
        pltpu.make_async_copy(dedges, out_edges, sems.at[10]),
        pltpu.make_async_copy(dstate, out_state, sems.at[11]),
    ]
    for copy in stores:
        copy.start()
    whole = packed[...] * FACTOR
    turned = jnp.concatenate([whole[0:128].T, whole[128:256].T], axis=1)
    o_w1[...] = turned[0:64, 0:192]
    o_nw1[...] = turned[64:128, 0:128]
    o_nw2[...] = whole[192:256, 0:64]
    o_w2[...] = pltpu.roll(whole[192:256], 64, 1)[:, 0:64]
    rows = turned[64:128, 128:192]
    for k, ref in enumerate((o_b1, o_eg, o_es, o_nb1, o_ng, o_ns)):
        ref[...] = rows[k : k + 1, :] + rows[k + 6 : k + 7, :]
    for k in range(10):
        copy = pltpu.make_async_copy(staged[k], results[k], sems.at[k])
        copy.start()
        stores.append(copy)
    for copy in stores:
        copy.wait()


def call(comm, *args):
    shapes = [
        ((D, NC), bf16),
        ((D, NF), bf16),
        ((64, 192), f32),
        ((1, 64), f32),
        ((64, 64), f32),
        ((1, 64), f32),
        ((1, 64), f32),
        ((64, 128), f32),
        ((1, 64), f32),
        ((64, 64), f32),
        ((1, 64), f32),
        ((1, 64), f32),
    ]
    dma = pltpu.SemaphoreType.DMA
    scratch = [pltpu.VMEM(arg.shape, arg.dtype) for arg in args]
    scratch += [
        pltpu.VMEM((256, NF), bf16),
        pltpu.VMEM((D, NF), f32),
        pltpu.VMEM((D, NF), f32),
        pltpu.VMEM((D, NF), f32),
        pltpu.VMEM((1, NF), f32),
        pltpu.VMEM((D, NF), bf16),
        pltpu.VMEM((128, NF), bf16),
        pltpu.VMEM((NF, 128), i16),
        pltpu.VMEM((NF, 128), i16),
        pltpu.VMEM((NB * HALO, 128), i16),
        pltpu.VMEM((NB, D, HALO), bf16),
        pltpu.VMEM((NB, D, HALO), bf16),
        pltpu.VMEM((NB, D, HALO), bf16),
        pltpu.VMEM((NB, D, HALO), bf16),
        pltpu.VMEM((192, NC), bf16),
        pltpu.VMEM((128, NC), bf16),
        pltpu.VMEM((D, NC), bf16),
        pltpu.VMEM((D, NC), f32),
        pltpu.VMEM((D, NC), f32),
        pltpu.VMEM((D, NB * HALO), f32),
        pltpu.VMEM((D, NC), f32),
        pltpu.VMEM((5, D, 128), f32),
        pltpu.VMEM((6, D, 128), f32),
        pltpu.VMEM((256, 128), f32),
        pltpu.VMEM((256, 128), bf16),
        pltpu.VMEM((8, 32, 128), bf16),
        pltpu.VMEM((16, 32, 128), bf16),
        pltpu.VMEM((8, 32, 128), bf16),
        pltpu.VMEM((192, 64), bf16),
        pltpu.VMEM((64, 64), bf16),
        pltpu.VMEM((128, 64), bf16),
        pltpu.VMEM((64, 64), bf16),
        dma((12,)), dma((12,)), dma((12,)), dma((12,)),
        dma((8,)), dma((8,)), dma((16,)), dma((16,)), dma((8,)), dma((8,)),
        dma((16,)),
    ]
    anywhere = pl.BlockSpec(memory_space=pltpu.HBM)
    params = dict(vmem_limit_bytes=36 * 1024 * 1024)
    if comm:
        params.update(collective_id=0, has_side_effects=True)
    vmem = pl.BlockSpec(memory_space=pltpu.VMEM)
    middle = pl.pallas_call(
        make_kernel(comm),
        out_shape=[
            jax.ShapeDtypeStruct(shape, kind) for shape, kind in shapes[:2] + [((256, 128), f32)]
        ],
        in_specs=[anywhere] * 16,
        out_specs=[vmem] * 3,
        scratch_shapes=scratch,
        compiler_params=pltpu.CompilerParams(**params),
        name="layer",
    )(*[pltpu.with_memory_space_constraint(arg, pltpu.HBM) for arg in args])
    return pl.pallas_call(
        finish,
        out_shape=[jax.ShapeDtypeStruct(shape, kind) for shape, kind in shapes],
        in_specs=[vmem] * 3,
        out_specs=[anywhere] * 12,
        scratch_shapes=[pltpu.VMEM(shape, kind) for shape, kind in shapes[2:]] + [dma((12,))],
        compiler_params=pltpu.CompilerParams(vmem_limit_bytes=8 * 1024 * 1024),
        name="finish",
    )(*middle)


def on_device(comm, node_state, edge_state, senders, receivers, send_index, node_cotangent, edge_cotangent,
              edge_first, edge_bias, edge_second, edge_gain, edge_shift, node_first, node_bias, node_second, node_gain):
    line = lambda v: v.reshape(1, -1)
    outs = call(
        comm, node_state, edge_state, line(senders), line(receivers), line(send_index),
        node_cotangent, edge_cotangent, edge_first.T, line(edge_bias), edge_second, line(edge_gain),
        line(edge_shift), node_first.T, line(node_bias), node_second, line(node_gain),
    )
    outs = [v.reshape(-1) if v.shape[0] == 1 else v for v in outs]
    outs[2] = outs[2].T
    outs[7] = outs[7].T
    return tuple(outs)


def solution(mesh):
    split = Mesh(mesh.devices.reshape(4, 4, 2, 4), AXES)
    every = P(None, AXES)
    in_specs = (every, every, P(AXES), P(AXES), P(AXES, None, None), every, every) + (P(),) * 9
    out_specs = (every, every) + (P(),) * 10
    return jax.shard_map(
        lambda *args: on_device(True, *args), mesh=split, in_specs=in_specs, out_specs=out_specs,
        check_vma=False,
    )
```

```python
import math

import jax
import jax.numpy as jnp
from jax import lax
from jax.experimental import pallas as pl
from jax.experimental.pallas import tpu as pltpu
from jax.sharding import Mesh
from jax.sharding import PartitionSpec as P

AXES = ("z", "y", "core", "sub")
MESH = pl.DeviceIdType.MESH
EPSILON = 1e-05
D = 64
NF = 3072
NC = 1024
NB = 12
HALO = 128
BLK = 512
bf16 = jnp.bfloat16
f32 = jnp.float32
i16 = jnp.int16
FACTOR = 1.0 / math.sqrt(393216)


def mm(a, b):
    return jnp.dot(a, b, preferred_element_type=f32)


def mm_last(a, b):
    return lax.dot_general(a, b, (((1,), (1,)), ((), ())), preferred_element_type=f32)


def rows_of(index):
    return jnp.broadcast_to(index, (16, index.shape[1])).astype(i16)


def selector(rows, tile):
    width = rows.shape[1]
    iota = lax.broadcasted_iota(jnp.int32, (256, 128), 0).astype(i16)
    iota = jnp.concatenate([iota] * (width // 128), axis=1)
    key = jnp.concatenate([rows - i16(256 * tile)] * 16, axis=0)
    return jnp.where(iota == key, bf16(1), bf16(0))


def columns_of(index):
    width = index.shape[1]
    sub = lax.broadcasted_iota(jnp.int32, (8, width), 0)
    low, high = index & 255, index >> 8
    parts = jnp.where(sub == 0, low, jnp.where(sub == 1, high, 0)).astype(f32)
    sub = lax.broadcasted_iota(jnp.int32, (8, 128), 0)
    scale = jnp.where(sub == 0, 1.0, jnp.where(sub == 1, 256.0, 0.0))
    out = lax.dot_general(parts, scale, (((0,), (0,)), ((), ())), preferred_element_type=f32)
    return out.astype(jnp.int32).astype(i16)


def selector_t(column, tile):
    lane = lax.broadcasted_iota(jnp.int32, (16, 128), 1).astype(i16)
    halves = []
    for half in range(2):
        key = jnp.concatenate([lane + i16(256 * tile + 128 * half)] * (column.shape[0] // 16), axis=0)
        halves.append(jnp.where(column == key, bf16(1), bf16(0)))
    return jnp.concatenate(halves, axis=1)


def staged(stages, count):
    for step in range(count + len(stages) - 1):
        for depth, stage in enumerate(stages):
            if 0 <= step - depth < count:
                stage(step - depth)


def block_at(i):
    return slice(i * BLK, i * BLK + BLK)


def column_of(row):
    sub = lax.broadcasted_iota(jnp.int32, (D, D), 0)
    lane = lax.broadcasted_iota(jnp.int32, (D, D), 1)
    col = jnp.sum(jnp.where(sub == lane, row, 0.0), axis=1, keepdims=True)
    return jnp.broadcast_to(col, (D, 128))


def wide(col, width):
    return jnp.concatenate([col] * (width // 128), axis=1)


def fold_lanes(values):
    total = values[:, 0:128]
    for begin in range(128, values.shape[1], 128):
        total = total + values[:, begin : begin + 128]
    return total


def mean_rows(values):
    return jnp.sum(values, axis=0, keepdims=True) * (1.0 / D)


def logistic(values):
    return 0.5 * jnp.tanh(0.5 * values) + 0.5


def standardize(values):
    centered = values - mean_rows(values)
    spread = lax.rsqrt(mean_rows(centered * centered) + EPSILON)
    return centered * spread, spread


def normalize_back(upstream, scaled, spread, gain):
    weighted = upstream * gain
    return spread * (weighted - mean_rows(weighted) - scaled * mean_rows(weighted * scaled))


def make_kernel(comm):
    def kernel(
        *refs
    ):
        given, refs = refs[:16], refs[16:]
        (dstate, dedges, packed), refs = refs[:3], refs[3:]
        held, refs = refs[:16], refs[16:]
        (
            stk, slope, scl, ups, spr, msg, ehd, col_s, col_r, col_p,
            sendb, ghost, gsend, gback, nin, nh2, nbr, own, acc, gac, gt,
            vec, sums, grads, shared, rs_buf, ex_buf, ag_buf, w1, w2t, nw1, nw2t,
            sem_fs, sem_fr, sem_bs, sem_br, sem_rs, sem_rr, sem_es, sem_er, sem_as, sem_ar,
            sem_in,
        ) = refs
        ns, es, snd, rcv, six, nct, ect, w1t, b1, w2, eg, esh, nw1t, nb1, nw2, ng = held
        loads = [
            pltpu.make_async_copy(given[k], held[k], sem_in.at[k]) for k in range(16)
        ]
        for k in (4, 0, 2, 3, 1, 7, 8, 9, 10, 11, 12, 13, 14, 15, 5, 6):
            loads[k].start()
        if comm:
            z = lax.axis_index("z")
            y = lax.axis_index("y")
            core = lax.axis_index("core")
            s = lax.axis_index("sub")
            d = z * 8 + y * 2 + core
            a = z * 2 + core
            b = y * 4 + s

            def row_peer(step, t):
                dd = lax.rem(d + (step + 32), 32)
                return lax.div(dd, 8), lax.rem(lax.div(dd, 2), 4), lax.rem(dd, 2), t

            def a_peer(j):
                other = lax.rem(a + j, 8)
                return other, (lax.div(other, 2), y, lax.rem(other, 2), s)

            def b_peer(j):
                other = lax.rem(b + j, 16)
                return other, (z, lax.div(other, 4), core, lax.rem(other, 4))

            halo_pairs = [(o, r) for o in range(3) for r in range(4) if not (o == 1 and r == 0)]
            barrier = pltpu.get_barrier_semaphore()
            peers = [row_peer(o - 1, lax.rem(s + r, 4)) for o, r in halo_pairs]
            peers += [a_peer(j)[1] for j in range(1, 8)] + [b_peer(j)[1] for j in range(1, 16)]
            for peer in peers:
                pl.semaphore_signal(barrier, inc=1, device_id=peer, device_id_type=MESH)
        else:
            s = 0

        def waits(copies):
            for condition, copy in copies:
                if condition is None:
                    copy.wait_send()
                else:
                    pl.when(condition)(copy.wait_send)

        def send_block(k, source, target, sems, turn):
            o, t = k // 4, k % 4
            copy = pltpu.make_async_remote_copy(
                src_ref=source.at[k],
                dst_ref=target.at[o * 4 + s],
                send_sem=sems[0].at[k],
                recv_sem=sems[1].at[o * 4 + s],
                device_id=row_peer(turn * (o - 1), t),
                device_id_type=MESH,
            )
            condition = s != t if o == 1 else None
            if condition is None:
                copy.start()
            else:
                pl.when(condition)(copy.start)
            return condition, copy

        def receive_blocks(source, target, sems):
            for o, r in halo_pairs:
                slot = o * 4 + lax.rem(s + r, 4)
                pltpu.make_async_remote_copy(
                    src_ref=source.at[slot],
                    dst_ref=target.at[slot],
                    send_sem=sems[0].at[0],
                    recv_sem=sems[1].at[slot],
                    device_id=row_peer(o - 1, lax.rem(s + r, 4)),
                    device_id_type=MESH,
                ).wait_recv()

        loads[4].wait()
        loads[0].wait()
        forward = []
        for place, pair in enumerate((0, 1, 4, 5, 2, 3)):
            rows = rows_of(six[:, 256 * pair : 256 * pair + 256])
            picked = jnp.zeros((D, 256), f32)
            for tile in range(4):
                picked = picked + mm(ns[:, 256 * tile : 256 * tile + 256], selector(rows, tile))
            picked = picked.astype(bf16)
            sendb[2 * pair] = picked[:, :HALO]
            sendb[2 * pair + 1] = picked[:, HALO:]
            if comm:
                if place == 0:
                    pl.semaphore_wait(barrier, len(peers))
                for k in (2 * pair, 2 * pair + 1):
                    forward.append(send_block(k, sendb, ghost, (sem_fs, sem_fr), 1))

        ghost[4 + s] = jnp.zeros((D, HALO), bf16)
        gback[4 + s] = jnp.zeros((D, HALO), bf16)
        for k in (2, 3, 1, 7, 8, 9, 10, 11, 12, 13, 14, 15):
            loads[k].wait()
        vec[0] = column_of(b1[...])
        vec[1] = column_of(eg[...])
        vec[2] = column_of(esh[...])
        vec[3] = column_of(nb1[...])
        vec[4] = column_of(ng[...])
        w1[...] = w1t[...].astype(f32).T.astype(bf16)
        w2t[...] = w2[...].astype(f32).T.astype(bf16)
        nw1[...] = nw1t[...].astype(f32).T.astype(bf16)
        nw2t[...] = nw2[...].astype(f32).T.astype(bf16)
        sums[...] = jnp.zeros_like(sums)
        stk[128:192, :] = es[...]
        nin[0:64, :] = ns[...]

        def gather_own(i):
            at = block_at(i)
            for index, begin in ((snd, 0), (rcv, 64)):
                rows = rows_of(index[:, at])
                total = jnp.zeros((D, BLK), f32)
                for tile in range(4):
                    total = total + mm(ns[:, 256 * tile : 256 * tile + 256], selector(rows, tile))
                stk[begin : begin + 64, at] = total.astype(bf16)
            col_r[at, :] = columns_of(rcv[:, at])

        staged([gather_own], NF // BLK)

        if comm:
            receive_blocks(sendb, ghost, (sem_fs, sem_fr))

        def gather_ghosts(i):
            at = block_at(i)
            rows = rows_of(snd[:, at])
            total = stk[0:64, at].astype(f32)
            for pair in range(NB // 2):
                table = jnp.concatenate([ghost[2 * pair], ghost[2 * pair + 1]], axis=1)
                total = total + mm(table, selector(rows, 4 + pair))
            stk[0:64, at] = total.astype(bf16)

        def forward_faces(i):
            at = block_at(i)
            linear = mm(w1t[...], stk[0:192, at]) + wide(vec[0], BLK)
            gate = logistic(linear)
            activated = linear * gate
            active = activated.astype(bf16)
            stk[192:256, at] = active
            slope[:, at] = gate + activated * (1.0 - gate)
            scaled, spread = standardize(mm(w2t[...], active))
            scl[:, at] = scaled
            spr[:, at] = spread
            msg[:, at] = (scaled * wide(vec[1], BLK) + wide(vec[2], BLK)).astype(bf16)

        def scatter(i, part, column, total, tiles, first):
            for tile in tiles:
                where = slice(256 * (tile - tiles[0]), 256 * (tile - tiles[0]) + 256)
                added = mm(part, selector_t(column, tile))
                total[:, where] = added if first else total[:, where] + added

        def sum_messages(i):
            at = block_at(i)
            scatter(i, msg[:, at], col_r[at, :], acc, range(4), i == 0)

        staged([gather_ghosts, forward_faces, sum_messages], NF // BLK)

        loads[5].wait()
        loads[6].wait()
        def cells(i):
            at = block_at(i)
            nin[64:128, at] = acc[:, at].astype(bf16)
            linear = mm(nw1t[...], nin[0:128, at]) + wide(vec[3], BLK)
            gate = logistic(linear)
            activated = linear * gate
            active = activated.astype(bf16)
            nin[128:192, at] = active
            scaled, spread = standardize(mm(nw2t[...], active))
            upstream = nct[:, at].astype(f32)
            sums[4] += fold_lanes(upstream * scaled)
            sums[5] += fold_lanes(upstream)
            delta = normalize_back(upstream, scaled, spread, wide(vec[4], BLK)).astype(bf16)
            nh2[0:64, at] = delta
            hidden = mm(nw2[...], delta) * (gate + activated * (1.0 - gate))
            sums[3] += fold_lanes(hidden)
            hidden = hidden.astype(bf16)
            nh2[64:128, at] = hidden
            back = mm(nw1[...], hidden)
            own[:, at] = back[0:64] + upstream
            nbr[:, at] = back[64:128].astype(bf16)

        staged([cells], NC // BLK)

        def gather_back(i):
            at = block_at(i)
            rows = rows_of(rcv[:, at])
            upstream = ect[:, at].astype(f32)
            for tile in range(4):
                upstream = upstream + mm(
                    nbr[:, 256 * tile : 256 * tile + 256], selector(rows, tile)
                )
            ups[:, at] = upstream

        def backward_faces(i):
            at = block_at(i)
            upstream = ups[:, at]
            scaled = scl[:, at]
            sums[1] += fold_lanes(upstream * scaled)
            sums[2] += fold_lanes(upstream)
            delta = normalize_back(upstream, scaled, spr[:, at], wide(vec[1], BLK)).astype(bf16)
            ehd[64:128, at] = delta
            hidden = mm(w2[...], delta) * slope[:, at]
            sums[0] += fold_lanes(hidden)
            ehd[0:64, at] = hidden.astype(bf16)

        staged([gather_back, backward_faces], NF // BLK)

        edge_part = mm_last(stk[...], ehd[...])
        node_part = mm_last(nin[...], nh2[...])
        lane64 = lax.broadcasted_iota(jnp.int32, (64, 128), 1)
        vectors = jnp.zeros((64, 128), f32)
        for number in range(6):
            vectors = jnp.where(
                lane64 == 64 + number, jnp.sum(sums[number], axis=1, keepdims=True), vectors
            )
        high = vectors.astype(bf16).astype(f32)
        vectors = high + pltpu.roll(vectors - high, 6, 1)
        grads[0:64] = jnp.where(lane64 < 64, edge_part[0:64], node_part[0:64])
        grads[64:128] = jnp.where(lane64 < 64, edge_part[64:128], node_part[64:128])
        grads[128:192] = jnp.where(lane64 < 64, edge_part[128:192], vectors)
        grads[192:256] = jnp.where(lane64 < 64, node_part[128:192], edge_part[192:256])

        first = []
        if comm:
            shared[...] = grads[...].astype(bf16)
            for j in range(1, 8):
                other, peer = a_peer(j)
                first.append(
                    pltpu.make_async_remote_copy(
                        src_ref=shared.at[pl.ds(pl.multiple_of(other * 32, 32), 32), :],
                        dst_ref=rs_buf.at[a],
                        send_sem=sem_rs.at[j],
                        recv_sem=sem_rr.at[a],
                        device_id=peer,
                        device_id_type=MESH,
                    )
                )
            for copy in first:
                copy.start()

        def sum_ghosts(i):
            at = block_at(i)
            col_s[at, :] = columns_of(snd[:, at])
            scatter(i, ehd[0:64, at], col_s[at, :], gac, range(4, 10), i == 0)

        staged([sum_ghosts], NF // BLK)
        def sum_senders(i):
            at = block_at(i)
            scatter(i, ehd[0:64, at], col_s[at, :], acc, range(4), i == 0)

        staged([sum_senders], NF // BLK)

        def split_vectors(total):
            lane = lax.broadcasted_iota(jnp.int32, (32, 128), 1)
            whole = total + pltpu.roll(total, 122, 1)
            high = whole.astype(bf16).astype(f32)
            parts = jnp.where(lane < 70, high, pltpu.roll(whole - high, 6, 1))
            return jnp.where(((a == 4) | (a == 5)) & (lane >= 64) & (lane < 76), parts, total)

        second = []
        if comm:
            total = grads[pl.ds(pl.multiple_of(a * 32, 32), 32), :]
            for j in range(1, 8):
                other, peer = a_peer(j)
                pltpu.make_async_remote_copy(
                    src_ref=rs_buf.at[other],
                    dst_ref=rs_buf.at[other],
                    send_sem=sem_rs.at[j],
                    recv_sem=sem_rr.at[other],
                    device_id=peer,
                    device_id_type=MESH,
                ).wait_recv()
                total = total + rs_buf[other].astype(f32)
            ex_buf[b] = split_vectors(total).astype(bf16)
            for j in range(1, 16):
                other, peer = b_peer(j)
                second.append(
                    pltpu.make_async_remote_copy(
                        src_ref=ex_buf.at[b],
                        dst_ref=ex_buf.at[b],
                        send_sem=sem_es.at[j],
                        recv_sem=sem_er.at[b],
                        device_id=peer,
                        device_id_type=MESH,
                    )
                )
            for copy in second:
                copy.start()

        backward = []
        for pair in (0, 1, 4, 5, 2, 3):
            block = mm(w1[0:64, :], gac[:, 256 * pair : 256 * pair + 256].astype(bf16)).astype(bf16)
            gsend[2 * pair] = block[:, :HALO]
            gsend[2 * pair + 1] = block[:, HALO:]
            if comm:
                for k in (2 * pair, 2 * pair + 1):
                    backward.append(send_block(k, gsend, gback, (sem_bs, sem_br), -1))

        def sum_receivers(i):
            at = block_at(i)
            scatter(i, ehd[0:64, at], col_r[at, :], gt, range(4), i == 0)

        staged([sum_receivers], NF // BLK)
        own[...] += mm(w1[0:64, :], acc[...].astype(bf16)) + mm(w1[64:128, :], gt[...].astype(bf16))
        for pair in range(NB // 2):
            at = slice(256 * pair, 256 * pair + 256)
            col_p[at, :] = columns_of(six[:, at])

        for i in range(NF // BLK):
            at = block_at(i)
            dedges[:, at] = (ect[:, at].astype(f32) + mm(w1[128:192, :], ehd[0:64, at])).astype(bf16)

        third = []
        if comm:
            for j in range(1, 16):
                other, peer = b_peer(j)
                pltpu.make_async_remote_copy(
                    src_ref=ex_buf.at[other],
                    dst_ref=ex_buf.at[other],
                    send_sem=sem_es.at[j],
                    recv_sem=sem_er.at[other],
                    device_id=peer,
                    device_id_type=MESH,
                ).wait_recv()
            total = ex_buf[0].astype(f32)
            for j in range(1, 16):
                total = total + ex_buf[j].astype(f32)
            ag_buf[a] = split_vectors(total).astype(bf16)
            for j in range(1, 8):
                other, peer = a_peer(j)
                third.append(
                    pltpu.make_async_remote_copy(
                        src_ref=ag_buf.at[a],
                        dst_ref=ag_buf.at[a],
                        send_sem=sem_as.at[j],
                        recv_sem=sem_ar.at[a],
                        device_id=peer,
                        device_id_type=MESH,
                    )
                )
            for copy in third:
                copy.start()

        if comm:
            receive_blocks(gsend, gback, (sem_bs, sem_br))

        returned = jnp.concatenate([gback[k] for k in range(NB)], axis=1)
        for tile in range(4):
            where = slice(256 * tile, 256 * tile + 256)
            total = own[:, where]
            for pair in range(NB // 2):
                at = slice(256 * pair, 256 * pair + 256)
                total = total + mm(returned[:, at], selector_t(col_p[at, :], tile))
            dstate[:, where] = total.astype(bf16)

        if comm:
            for j in range(1, 8):
                other, peer = a_peer(j)
                pltpu.make_async_remote_copy(
                    src_ref=ag_buf.at[other],
                    dst_ref=ag_buf.at[other],
                    send_sem=sem_as.at[j],
                    recv_sem=sem_ar.at[other],
                    device_id=peer,
                    device_id_type=MESH,
                ).wait_recv()
            for j in range(8):
                packed[32 * j : 32 * j + 32] = ag_buf[j].astype(f32)
        else:
            packed[...] = grads[...]
        waits(forward + backward)
        for copy in first + second + third:
            copy.wait_send()

    return kernel


def finish(
    dstate, dedges, packed, out_state, out_edges, *refs
):
    results, refs = refs[:10], refs[10:]
    staged, sems = refs[:10], refs[10]
    o_w1, o_b1, o_w2, o_eg, o_es, o_nw1, o_nb1, o_nw2, o_ng, o_ns = staged
    stores = [
        pltpu.make_async_copy(dedges, out_edges, sems.at[10]),
        pltpu.make_async_copy(dstate, out_state, sems.at[11]),
    ]
    for copy in stores:
        copy.start()
    whole = packed[...] * FACTOR
    turned = jnp.concatenate([whole[0:128].T, whole[128:256].T], axis=1)
    o_w1[...] = turned[0:64, 0:192]
    o_nw1[...] = turned[64:128, 0:128]
    o_nw2[...] = whole[192:256, 0:64]
    o_w2[...] = pltpu.roll(whole[192:256], 64, 1)[:, 0:64]
    rows = turned[64:128, 128:192]
    for k, ref in enumerate((o_b1, o_eg, o_es, o_nb1, o_ng, o_ns)):
        ref[...] = rows[k : k + 1, :] + rows[k + 6 : k + 7, :]
    for k in range(10):
        copy = pltpu.make_async_copy(staged[k], results[k], sems.at[k])
        copy.start()
        stores.append(copy)
    for copy in stores:
        copy.wait()


def call(comm, *args):
    shapes = [
        ((D, NC), bf16),
        ((D, NF), bf16),
        ((64, 192), f32),
        ((1, 64), f32),
        ((64, 64), f32),
        ((1, 64), f32),
        ((1, 64), f32),
        ((64, 128), f32),
        ((1, 64), f32),
        ((64, 64), f32),
        ((1, 64), f32),
        ((1, 64), f32),
    ]
    dma = pltpu.SemaphoreType.DMA
    scratch = [pltpu.VMEM(arg.shape, arg.dtype) for arg in args]
    scratch += [
        pltpu.VMEM((256, NF), bf16),
        pltpu.VMEM((D, NF), f32),
        pltpu.VMEM((D, NF), f32),
        pltpu.VMEM((D, NF), f32),
        pltpu.VMEM((1, NF), f32),
        pltpu.VMEM((D, NF), bf16),
        pltpu.VMEM((128, NF), bf16),
        pltpu.VMEM((NF, 128), i16),
        pltpu.VMEM((NF, 128), i16),
        pltpu.VMEM((NB * HALO, 128), i16),
        pltpu.VMEM((NB, D, HALO), bf16),
        pltpu.VMEM((NB, D, HALO), bf16),
        pltpu.VMEM((NB, D, HALO), bf16),
        pltpu.VMEM((NB, D, HALO), bf16),
        pltpu.VMEM((192, NC), bf16),
        pltpu.VMEM((128, NC), bf16),
        pltpu.VMEM((D, NC), bf16),
        pltpu.VMEM((D, NC), f32),
        pltpu.VMEM((D, NC), f32),
        pltpu.VMEM((D, NB * HALO), f32),
        pltpu.VMEM((D, NC), f32),
        pltpu.VMEM((5, D, 128), f32),
        pltpu.VMEM((6, D, 128), f32),
        pltpu.VMEM((256, 128), f32),
        pltpu.VMEM((256, 128), bf16),
        pltpu.VMEM((8, 32, 128), bf16),
        pltpu.VMEM((16, 32, 128), bf16),
        pltpu.VMEM((8, 32, 128), bf16),
        pltpu.VMEM((192, 64), bf16),
        pltpu.VMEM((64, 64), bf16),
        pltpu.VMEM((128, 64), bf16),
        pltpu.VMEM((64, 64), bf16),
        dma((12,)), dma((12,)), dma((12,)), dma((12,)),
        dma((8,)), dma((8,)), dma((16,)), dma((16,)), dma((8,)), dma((8,)),
        dma((16,)),
    ]
    anywhere = pl.BlockSpec(memory_space=pltpu.HBM)
    params = dict(vmem_limit_bytes=36 * 1024 * 1024)
    if comm:
        params.update(collective_id=0, has_side_effects=True)
    vmem = pl.BlockSpec(memory_space=pltpu.VMEM)
    middle = pl.pallas_call(
        make_kernel(comm),
        out_shape=[
            jax.ShapeDtypeStruct(shape, kind) for shape, kind in shapes[:2] + [((256, 128), f32)]
        ],
        in_specs=[anywhere] * 16,
        out_specs=[vmem] * 3,
        scratch_shapes=scratch,
        compiler_params=pltpu.CompilerParams(**params),
        name="layer",
    )(*[pltpu.with_memory_space_constraint(arg, pltpu.HBM) for arg in args])
    return pl.pallas_call(
        finish,
        out_shape=[jax.ShapeDtypeStruct(shape, kind) for shape, kind in shapes],
        in_specs=[vmem] * 3,
        out_specs=[anywhere] * 12,
        scratch_shapes=[pltpu.VMEM(shape, kind) for shape, kind in shapes[2:]] + [dma((12,))],
        compiler_params=pltpu.CompilerParams(vmem_limit_bytes=8 * 1024 * 1024),
        name="finish",
    )(*middle)


def on_device(comm, node_state, edge_state, senders, receivers, send_index, node_cotangent, edge_cotangent,
              edge_first, edge_bias, edge_second, edge_gain, edge_shift, node_first, node_bias, node_second, node_gain):
    line = lambda v: v.reshape(1, -1)
    outs = call(
        comm, node_state, edge_state, line(senders), line(receivers), line(send_index),
        node_cotangent, edge_cotangent, edge_first.T, line(edge_bias), edge_second, line(edge_gain),
        line(edge_shift), node_first.T, line(node_bias), node_second, line(node_gain),
    )
    outs = [v.reshape(-1) if v.shape[0] == 1 else v for v in outs]
    outs[2] = outs[2].T
    outs[7] = outs[7].T
    return tuple(outs)


def solution(mesh):
    split = Mesh(mesh.devices.reshape(4, 4, 2, 4), AXES)
    every = P(None, AXES)
    in_specs = (every, every, P(AXES), P(AXES), P(AXES, None, None), every, every) + (P(),) * 9
    out_specs = (every, every) + (P(),) * 10
    return jax.shard_map(
        lambda *args: on_device(True, *args), mesh=split, in_specs=in_specs, out_specs=out_specs,
        check_vma=False,
    )
```

```python
import math

import jax
import jax.numpy as jnp
from jax import lax
from jax.experimental import pallas as pl
from jax.experimental.pallas import tpu as pltpu
from jax.sharding import Mesh
from jax.sharding import PartitionSpec as P

AXES = ("z", "y", "core", "sub")
MESH = pl.DeviceIdType.MESH
EPSILON = 1e-05
D = 64
NF = 3072
NC = 1024
NB = 12
HALO = 128
BLK = 512
bf16 = jnp.bfloat16
f32 = jnp.float32
i16 = jnp.int16
FACTOR = 1.0 / math.sqrt(393216)


def mm(a, b):
    return jnp.dot(a, b, preferred_element_type=f32)


def mm_last(a, b):
    return lax.dot_general(a, b, (((1,), (1,)), ((), ())), preferred_element_type=f32)


def rows_of(index):
    return jnp.broadcast_to(index, (16, index.shape[1])).astype(i16)


def selector(rows, tile):
    width = rows.shape[1]
    iota = lax.broadcasted_iota(jnp.int32, (256, 128), 0).astype(i16)
    iota = jnp.concatenate([iota] * (width // 128), axis=1)
    key = jnp.concatenate([rows - i16(256 * tile)] * 16, axis=0)
    return jnp.where(iota == key, bf16(1), bf16(0))


def columns_of(index):
    width = index.shape[1]
    sub = lax.broadcasted_iota(jnp.int32, (8, width), 0)
    low, high = index & 255, index >> 8
    parts = jnp.where(sub == 0, low, jnp.where(sub == 1, high, 0)).astype(f32)
    sub = lax.broadcasted_iota(jnp.int32, (8, 128), 0)
    scale = jnp.where(sub == 0, 1.0, jnp.where(sub == 1, 256.0, 0.0))
    out = lax.dot_general(parts, scale, (((0,), (0,)), ((), ())), preferred_element_type=f32)
    return out.astype(jnp.int32).astype(i16)


def selector_t(column, tile):
    lane = lax.broadcasted_iota(jnp.int32, (16, 128), 1).astype(i16)
    halves = []
    for half in range(2):
        key = jnp.concatenate([lane + i16(256 * tile + 128 * half)] * (column.shape[0] // 16), axis=0)
        halves.append(jnp.where(column == key, bf16(1), bf16(0)))
    return jnp.concatenate(halves, axis=1)


def staged(stages, count):
    for step in range(count + len(stages) - 1):
        for depth, stage in enumerate(stages):
            if 0 <= step - depth < count:
                stage(step - depth)


def block_at(i):
    return slice(i * BLK, i * BLK + BLK)


def column_of(row):
    sub = lax.broadcasted_iota(jnp.int32, (D, D), 0)
    lane = lax.broadcasted_iota(jnp.int32, (D, D), 1)
    col = jnp.sum(jnp.where(sub == lane, row, 0.0), axis=1, keepdims=True)
    return jnp.broadcast_to(col, (D, 128))


def wide(col, width):
    return jnp.concatenate([col] * (width // 128), axis=1)


def fold_lanes(values):
    total = values[:, 0:128]
    for begin in range(128, values.shape[1], 128):
        total = total + values[:, begin : begin + 128]
    return total


def mean_rows(values):
    return jnp.sum(values, axis=0, keepdims=True) * (1.0 / D)


def logistic(values):
    return 0.5 * jnp.tanh(0.5 * values) + 0.5


def standardize(values):
    centered = values - mean_rows(values)
    spread = lax.rsqrt(mean_rows(centered * centered) + EPSILON)
    return centered * spread, spread


def normalize_back(upstream, scaled, spread, gain):
    weighted = upstream * gain
    return spread * (weighted - mean_rows(weighted) - scaled * mean_rows(weighted * scaled))


def make_kernel(comm):
    def kernel(
        *refs
    ):
        given, refs = refs[:16], refs[16:]
        (dstate, dedges, packed), refs = refs[:3], refs[3:]
        held, refs = refs[:16], refs[16:]
        (
            stk, slope, scl, ups, spr, msg, ehd, col_s, col_r, col_p,
            sendb, ghost, gsend, gback, nin, nh2, nbr, own, nslope, acc, gac, gt,
            vec, sums, grads, eacc, shared, rs_buf, ex_buf, ag_buf, w1, w2t, nw1, nw2t,
            sem_fs, sem_fr, sem_bs, sem_br, sem_rs, sem_rr, sem_es, sem_er, sem_as, sem_ar,
            sem_in,
        ) = refs
        ns, es, snd, rcv, six, nct, ect, w1t, b1, w2, eg, esh, nw1t, nb1, nw2, ng = held
        loads = [
            pltpu.make_async_copy(given[k], held[k], sem_in.at[k]) for k in range(16)
        ]
        for k in (4, 0, 2, 3, 1, 7, 8, 9, 10, 11, 12, 13, 14, 15, 5, 6):
            loads[k].start()
        if comm:
            z = lax.axis_index("z")
            y = lax.axis_index("y")
            core = lax.axis_index("core")
            s = lax.axis_index("sub")
            d = z * 8 + y * 2 + core
            a = z * 2 + core
            b = y * 4 + s

            def row_peer(step, t):
                dd = lax.rem(d + (step + 32), 32)
                return lax.div(dd, 8), lax.rem(lax.div(dd, 2), 4), lax.rem(dd, 2), t

            def a_peer(j):
                other = lax.rem(a + j, 8)
                return other, (lax.div(other, 2), y, lax.rem(other, 2), s)

            def b_peer(j):
                other = lax.rem(b + j, 16)
                return other, (z, lax.div(other, 4), core, lax.rem(other, 4))

            halo_pairs = [(o, r) for o in range(3) for r in range(4) if not (o == 1 and r == 0)]
            barrier = pltpu.get_barrier_semaphore()
            peers = [row_peer(o - 1, lax.rem(s + r, 4)) for o, r in halo_pairs]
            peers += [a_peer(j)[1] for j in range(1, 8)] + [b_peer(j)[1] for j in range(1, 16)]
            for peer in peers:
                pl.semaphore_signal(barrier, inc=1, device_id=peer, device_id_type=MESH)
        else:
            s = 0

        def waits(copies):
            for condition, copy in copies:
                if condition is None:
                    copy.wait_send()
                else:
                    pl.when(condition)(copy.wait_send)

        def send_block(k, source, target, sems, turn):
            o, t = k // 4, k % 4
            copy = pltpu.make_async_remote_copy(
                src_ref=source.at[k],
                dst_ref=target.at[o * 4 + s],
                send_sem=sems[0].at[k],
                recv_sem=sems[1].at[o * 4 + s],
                device_id=row_peer(turn * (o - 1), t),
                device_id_type=MESH,
            )
            condition = s != t if o == 1 else None
            if condition is None:
                copy.start()
            else:
                pl.when(condition)(copy.start)
            return condition, copy

        def receive_blocks(source, target, sems):
            for o, r in halo_pairs:
                slot = o * 4 + lax.rem(s + r, 4)
                pltpu.make_async_remote_copy(
                    src_ref=source.at[slot],
                    dst_ref=target.at[slot],
                    send_sem=sems[0].at[0],
                    recv_sem=sems[1].at[slot],
                    device_id=row_peer(o - 1, lax.rem(s + r, 4)),
                    device_id_type=MESH,
                ).wait_recv()

        loads[4].wait()
        loads[0].wait()
        forward = []
        for place, pair in enumerate((0, 1, 4, 5, 2, 3)):
            rows = rows_of(six[:, 256 * pair : 256 * pair + 256])
            picked = jnp.zeros((D, 256), f32)
            for tile in range(4):
                picked = picked + mm(ns[:, 256 * tile : 256 * tile + 256], selector(rows, tile))
            picked = picked.astype(bf16)
            sendb[2 * pair] = picked[:, :HALO]
            sendb[2 * pair + 1] = picked[:, HALO:]
            if comm:
                if place == 0:
                    pl.semaphore_wait(barrier, len(peers))
                for k in (2 * pair, 2 * pair + 1):
                    forward.append(send_block(k, sendb, ghost, (sem_fs, sem_fr), 1))

        ghost[4 + s] = jnp.zeros((D, HALO), bf16)
        gback[4 + s] = jnp.zeros((D, HALO), bf16)
        for k in (2, 3, 1, 7, 8, 9, 10, 11, 12, 13, 14, 15):
            loads[k].wait()
        vec[0] = column_of(b1[...])
        vec[1] = column_of(eg[...])
        vec[2] = column_of(esh[...])
        vec[3] = column_of(nb1[...])
        vec[4] = column_of(ng[...])
        w1[...] = w1t[...].astype(f32).T.astype(bf16)
        w2t[...] = w2[...].astype(f32).T.astype(bf16)
        nw1[...] = nw1t[...].astype(f32).T.astype(bf16)
        nw2t[...] = nw2[...].astype(f32).T.astype(bf16)
        sums[...] = jnp.zeros_like(sums)
        stk[128:192, :] = es[...]
        nin[0:64, :] = ns[...]

        def gather_own(i):
            at = block_at(i)
            for index, begin in ((snd, 0), (rcv, 64)):
                rows = rows_of(index[:, at])
                total = jnp.zeros((D, BLK), f32)
                for tile in range(4):
                    total = total + mm(ns[:, 256 * tile : 256 * tile + 256], selector(rows, tile))
                stk[begin : begin + 64, at] = total.astype(bf16)
            col_r[at, :] = columns_of(rcv[:, at])
            col_s[at, :] = columns_of(snd[:, at])

        staged([gather_own], NF // BLK)
        for pair in range(NB // 2):
            at = slice(256 * pair, 256 * pair + 256)
            col_p[at, :] = columns_of(six[:, at])

        if comm:
            receive_blocks(sendb, ghost, (sem_fs, sem_fr))

        def gather_ghosts(i):
            at = block_at(i)
            rows = rows_of(snd[:, at])
            total = stk[0:64, at].astype(f32)
            for pair in range(NB // 2):
                table = jnp.concatenate([ghost[2 * pair], ghost[2 * pair + 1]], axis=1)
                total = total + mm(table, selector(rows, 4 + pair))
            stk[0:64, at] = total.astype(bf16)

        def forward_faces(i):
            at = block_at(i)
            linear = mm(w1t[...], stk[0:192, at]) + wide(vec[0], BLK)
            gate = logistic(linear)
            activated = linear * gate
            active = activated.astype(bf16)
            stk[192:256, at] = active
            slope[:, at] = gate + activated * (1.0 - gate)

        def forward_norms(i):
            at = block_at(i)
            scaled, spread = standardize(mm(w2t[...], stk[192:256, at]))
            scl[:, at] = scaled
            spr[:, at] = spread
            msg[:, at] = (scaled * wide(vec[1], BLK) + wide(vec[2], BLK)).astype(bf16)

        def scatter(i, part, column, total, tiles, first):
            for tile in tiles:
                where = slice(256 * (tile - tiles[0]), 256 * (tile - tiles[0]) + 256)
                added = mm(part, selector_t(column, tile))
                total[:, where] = added if first else total[:, where] + added

        def sum_messages(i):
            at = block_at(i)
            scatter(i, msg[:, at], col_r[at, :], acc, range(4), i == 0)

        staged([gather_ghosts, forward_faces, forward_norms, sum_messages], NF // BLK)

        loads[5].wait()
        loads[6].wait()
        def cells(i):
            at = block_at(i)
            nin[64:128, at] = acc[:, at].astype(bf16)
            linear = mm(nw1t[...], nin[0:128, at]) + wide(vec[3], BLK)
            gate = logistic(linear)
            activated = linear * gate
            active = activated.astype(bf16)
            nin[128:192, at] = active
            nslope[:, at] = gate + activated * (1.0 - gate)

        def cell_norms(i):
            at = block_at(i)
            scaled, spread = standardize(mm(nw2t[...], nin[128:192, at]))
            upstream = nct[:, at].astype(f32)
            sums[4] += fold_lanes(upstream * scaled)
            sums[5] += fold_lanes(upstream)
            delta = normalize_back(upstream, scaled, spread, wide(vec[4], BLK)).astype(bf16)
            nh2[0:64, at] = delta

        def cell_hidden(i):
            at = block_at(i)
            upstream = nct[:, at].astype(f32)
            hidden = mm(nw2[...], nh2[0:64, at]) * nslope[:, at]
            sums[3] += fold_lanes(hidden)
            hidden = hidden.astype(bf16)
            nh2[64:128, at] = hidden
            back = mm(nw1[...], hidden)
            own[:, at] = back[0:64] + upstream
            nbr[:, at] = back[64:128].astype(bf16)

        staged([cells, cell_norms, cell_hidden], NC // BLK)

        def gather_back(i):
            at = block_at(i)
            rows = rows_of(rcv[:, at])
            upstream = ect[:, at].astype(f32)
            for tile in range(4):
                upstream = upstream + mm(
                    nbr[:, 256 * tile : 256 * tile + 256], selector(rows, tile)
                )
            ups[:, at] = upstream

        def backward_faces(i):
            at = block_at(i)
            upstream = ups[:, at]
            scaled = scl[:, at]
            sums[1] += fold_lanes(upstream * scaled)
            sums[2] += fold_lanes(upstream)
            delta = normalize_back(upstream, scaled, spr[:, at], wide(vec[1], BLK)).astype(bf16)
            ehd[64:128, at] = delta

        def backward_hidden(i):
            at = block_at(i)
            hidden = mm(w2[...], ehd[64:128, at]) * slope[:, at]
            sums[0] += fold_lanes(hidden)
            ehd[0:64, at] = hidden.astype(bf16)

        def weigh_faces(i):
            at = block_at(i)
            part = mm_last(stk[:, at], ehd[:, at])
            eacc[...] = part if i == 0 else eacc[...] + part

        staged([gather_back, backward_faces, backward_hidden, weigh_faces], NF // BLK)

        edge_part = eacc[...]
        node_part = mm_last(nin[...], nh2[...])
        lane64 = lax.broadcasted_iota(jnp.int32, (64, 128), 1)
        vectors = jnp.zeros((64, 128), f32)
        for number in range(6):
            vectors = jnp.where(
                lane64 == 64 + number, jnp.sum(sums[number], axis=1, keepdims=True), vectors
            )
        high = vectors.astype(bf16).astype(f32)
        vectors = high + pltpu.roll(vectors - high, 6, 1)
        grads[0:64] = jnp.where(lane64 < 64, edge_part[0:64], node_part[0:64])
        grads[64:128] = jnp.where(lane64 < 64, edge_part[64:128], node_part[64:128])
        grads[128:192] = jnp.where(lane64 < 64, edge_part[128:192], vectors)
        grads[192:256] = jnp.where(lane64 < 64, node_part[128:192], edge_part[192:256])

        first = []
        if comm:
            shared[...] = grads[...].astype(bf16)
            for j in range(1, 8):
                other, peer = a_peer(j)
                first.append(
                    pltpu.make_async_remote_copy(
                        src_ref=shared.at[pl.ds(pl.multiple_of(other * 32, 32), 32), :],
                        dst_ref=rs_buf.at[a],
                        send_sem=sem_rs.at[j],
                        recv_sem=sem_rr.at[a],
                        device_id=peer,
                        device_id_type=MESH,
                    )
                )
            for copy in first:
                copy.start()

        def sum_ghosts(i):
            at = block_at(i)
            scatter(i, ehd[0:64, at], col_s[at, :], gac, range(4, 10), i == 0)

        staged([sum_ghosts], NF // BLK)
        def sum_senders(i):
            at = block_at(i)
            scatter(i, ehd[0:64, at], col_s[at, :], acc, range(4), i == 0)

        staged([sum_senders], NF // BLK)

        def split_vectors(total):
            lane = lax.broadcasted_iota(jnp.int32, (32, 128), 1)
            whole = total + pltpu.roll(total, 122, 1)
            high = whole.astype(bf16).astype(f32)
            parts = jnp.where(lane < 70, high, pltpu.roll(whole - high, 6, 1))
            return jnp.where(((a == 4) | (a == 5)) & (lane >= 64) & (lane < 76), parts, total)

        second = []
        if comm:
            total = grads[pl.ds(pl.multiple_of(a * 32, 32), 32), :]
            for j in range(1, 8):
                other, peer = a_peer(j)
                pltpu.make_async_remote_copy(
                    src_ref=rs_buf.at[other],
                    dst_ref=rs_buf.at[other],
                    send_sem=sem_rs.at[j],
                    recv_sem=sem_rr.at[other],
                    device_id=peer,
                    device_id_type=MESH,
                ).wait_recv()
                total = total + rs_buf[other].astype(f32)
            ex_buf[b] = split_vectors(total).astype(bf16)
            for j in range(1, 16):
                other, peer = b_peer(j)
                second.append(
                    pltpu.make_async_remote_copy(
                        src_ref=ex_buf.at[b],
                        dst_ref=ex_buf.at[b],
                        send_sem=sem_es.at[j],
                        recv_sem=sem_er.at[b],
                        device_id=peer,
                        device_id_type=MESH,
                    )
                )
            for copy in second:
                copy.start()

        backward = []
        for pair in (0, 1, 4, 5, 2, 3):
            block = mm(w1[0:64, :], gac[:, 256 * pair : 256 * pair + 256].astype(bf16)).astype(bf16)
            gsend[2 * pair] = block[:, :HALO]
            gsend[2 * pair + 1] = block[:, HALO:]
            if comm:
                for k in (2 * pair, 2 * pair + 1):
                    backward.append(send_block(k, gsend, gback, (sem_bs, sem_br), -1))

        def sum_receivers(i):
            at = block_at(i)
            scatter(i, ehd[0:64, at], col_r[at, :], gt, range(4), i == 0)

        staged([sum_receivers], NF // BLK)
        own[...] += mm(w1[0:64, :], acc[...].astype(bf16)) + mm(w1[64:128, :], gt[...].astype(bf16))

        for i in range(NF // BLK):
            at = block_at(i)
            dedges[:, at] = (ect[:, at].astype(f32) + mm(w1[128:192, :], ehd[0:64, at])).astype(bf16)

        third = []
        if comm:
            for j in range(1, 16):
                other, peer = b_peer(j)
                pltpu.make_async_remote_copy(
                    src_ref=ex_buf.at[other],
                    dst_ref=ex_buf.at[other],
                    send_sem=sem_es.at[j],
                    recv_sem=sem_er.at[other],
                    device_id=peer,
                    device_id_type=MESH,
                ).wait_recv()
            total = ex_buf[0].astype(f32)
            for j in range(1, 16):
                total = total + ex_buf[j].astype(f32)
            ag_buf[a] = split_vectors(total).astype(bf16)
            for j in range(1, 8):
                other, peer = a_peer(j)
                third.append(
                    pltpu.make_async_remote_copy(
                        src_ref=ag_buf.at[a],
                        dst_ref=ag_buf.at[a],
                        send_sem=sem_as.at[j],
                        recv_sem=sem_ar.at[a],
                        device_id=peer,
                        device_id_type=MESH,
                    )
                )
            for copy in third:
                copy.start()

        if comm:
            receive_blocks(gsend, gback, (sem_bs, sem_br))

        returned = jnp.concatenate([gback[k] for k in range(NB)], axis=1)
        for tile in range(4):
            where = slice(256 * tile, 256 * tile + 256)
            total = own[:, where]
            for pair in range(NB // 2):
                at = slice(256 * pair, 256 * pair + 256)
                total = total + mm(returned[:, at], selector_t(col_p[at, :], tile))
            dstate[:, where] = total.astype(bf16)

        if comm:
            for j in range(1, 8):
                other, peer = a_peer(j)
                pltpu.make_async_remote_copy(
                    src_ref=ag_buf.at[other],
                    dst_ref=ag_buf.at[other],
                    send_sem=sem_as.at[j],
                    recv_sem=sem_ar.at[other],
                    device_id=peer,
                    device_id_type=MESH,
                ).wait_recv()
            for j in range(8):
                packed[32 * j : 32 * j + 32] = ag_buf[j].astype(f32)
        else:
            packed[...] = grads[...]
        waits(forward + backward)
        for copy in first + second + third:
            copy.wait_send()

    return kernel


def finish(
    dstate, dedges, packed, out_state, out_edges, *refs
):
    results, refs = refs[:10], refs[10:]
    staged, sems = refs[:10], refs[10]
    o_w1, o_b1, o_w2, o_eg, o_es, o_nw1, o_nb1, o_nw2, o_ng, o_ns = staged
    stores = [
        pltpu.make_async_copy(dedges, out_edges, sems.at[10]),
        pltpu.make_async_copy(dstate, out_state, sems.at[11]),
    ]
    for copy in stores:
        copy.start()
    whole = packed[...] * FACTOR
    turned = jnp.concatenate([whole[0:128].T, whole[128:256].T], axis=1)
    o_w1[...] = turned[0:64, 0:192]
    o_nw1[...] = turned[64:128, 0:128]
    o_nw2[...] = whole[192:256, 0:64]
    o_w2[...] = pltpu.roll(whole[192:256], 64, 1)[:, 0:64]
    rows = turned[64:128, 128:192]
    for k, ref in enumerate((o_b1, o_eg, o_es, o_nb1, o_ng, o_ns)):
        ref[...] = rows[k : k + 1, :] + rows[k + 6 : k + 7, :]
    for k in range(10):
        copy = pltpu.make_async_copy(staged[k], results[k], sems.at[k])
        copy.start()
        stores.append(copy)
    for copy in stores:
        copy.wait()


def call(comm, *args):
    shapes = [
        ((D, NC), bf16),
        ((D, NF), bf16),
        ((64, 192), f32),
        ((1, 64), f32),
        ((64, 64), f32),
        ((1, 64), f32),
        ((1, 64), f32),
        ((64, 128), f32),
        ((1, 64), f32),
        ((64, 64), f32),
        ((1, 64), f32),
        ((1, 64), f32),
    ]
    dma = pltpu.SemaphoreType.DMA
    scratch = [pltpu.VMEM(arg.shape, arg.dtype) for arg in args]
    scratch += [
        pltpu.VMEM((256, NF), bf16),
        pltpu.VMEM((D, NF), f32),
        pltpu.VMEM((D, NF), f32),
        pltpu.VMEM((D, NF), f32),
        pltpu.VMEM((1, NF), f32),
        pltpu.VMEM((D, NF), bf16),
        pltpu.VMEM((128, NF), bf16),
        pltpu.VMEM((NF, 128), i16),
        pltpu.VMEM((NF, 128), i16),
        pltpu.VMEM((NB * HALO, 128), i16),
        pltpu.VMEM((NB, D, HALO), bf16),
        pltpu.VMEM((NB, D, HALO), bf16),
        pltpu.VMEM((NB, D, HALO), bf16),
        pltpu.VMEM((NB, D, HALO), bf16),
        pltpu.VMEM((192, NC), bf16),
        pltpu.VMEM((128, NC), bf16),
        pltpu.VMEM((D, NC), bf16),
        pltpu.VMEM((D, NC), f32),
        pltpu.VMEM((D, NC), f32),
        pltpu.VMEM((D, NC), f32),
        pltpu.VMEM((D, NB * HALO), f32),
        pltpu.VMEM((D, NC), f32),
        pltpu.VMEM((5, D, 128), f32),
        pltpu.VMEM((6, D, 128), f32),
        pltpu.VMEM((256, 128), f32),
        pltpu.VMEM((256, 128), f32),
        pltpu.VMEM((256, 128), bf16),
        pltpu.VMEM((8, 32, 128), bf16),
        pltpu.VMEM((16, 32, 128), bf16),
        pltpu.VMEM((8, 32, 128), bf16),
        pltpu.VMEM((192, 64), bf16),
        pltpu.VMEM((64, 64), bf16),
        pltpu.VMEM((128, 64), bf16),
        pltpu.VMEM((64, 64), bf16),
        dma((12,)), dma((12,)), dma((12,)), dma((12,)),
        dma((8,)), dma((8,)), dma((16,)), dma((16,)), dma((8,)), dma((8,)),
        dma((16,)),
    ]
    anywhere = pl.BlockSpec(memory_space=pltpu.HBM)
    params = dict(vmem_limit_bytes=36 * 1024 * 1024)
    if comm:
        params.update(collective_id=0, has_side_effects=True)
    vmem = pl.BlockSpec(memory_space=pltpu.VMEM)
    middle = pl.pallas_call(
        make_kernel(comm),
        out_shape=[
            jax.ShapeDtypeStruct(shape, kind) for shape, kind in shapes[:2] + [((256, 128), f32)]
        ],
        in_specs=[anywhere] * 16,
        out_specs=[vmem] * 3,
        scratch_shapes=scratch,
        compiler_params=pltpu.CompilerParams(**params),
        name="layer",
    )(*[pltpu.with_memory_space_constraint(arg, pltpu.HBM) for arg in args])
    return pl.pallas_call(
        finish,
        out_shape=[jax.ShapeDtypeStruct(shape, kind) for shape, kind in shapes],
        in_specs=[vmem] * 3,
        out_specs=[anywhere] * 12,
        scratch_shapes=[pltpu.VMEM(shape, kind) for shape, kind in shapes[2:]] + [dma((12,))],
        compiler_params=pltpu.CompilerParams(vmem_limit_bytes=8 * 1024 * 1024),
        name="finish",
    )(*middle)


def on_device(comm, node_state, edge_state, senders, receivers, send_index, node_cotangent, edge_cotangent,
              edge_first, edge_bias, edge_second, edge_gain, edge_shift, node_first, node_bias, node_second, node_gain):
    line = lambda v: v.reshape(1, -1)
    outs = call(
        comm, node_state, edge_state, line(senders), line(receivers), line(send_index),
        node_cotangent, edge_cotangent, edge_first.T, line(edge_bias), edge_second, line(edge_gain),
        line(edge_shift), node_first.T, line(node_bias), node_second, line(node_gain),
    )
    outs = [v.reshape(-1) if v.shape[0] == 1 else v for v in outs]
    outs[2] = outs[2].T
    outs[7] = outs[7].T
    return tuple(outs)


def solution(mesh):
    split = Mesh(mesh.devices.reshape(4, 4, 2, 4), AXES)
    every = P(None, AXES)
    in_specs = (every, every, P(AXES), P(AXES), P(AXES, None, None), every, every) + (P(),) * 9
    out_specs = (every, every) + (P(),) * 10
    return jax.shard_map(
        lambda *args: on_device(True, *args), mesh=split, in_specs=in_specs, out_specs=out_specs,
        check_vma=False,
    )
```

```python
import math

import jax
import jax.numpy as jnp
from jax import lax
from jax.experimental import pallas as pl
from jax.experimental.pallas import tpu as pltpu
from jax.sharding import Mesh
from jax.sharding import PartitionSpec as P

AXES = ("z", "y", "core", "sub")
MESH = pl.DeviceIdType.MESH
EPSILON = 1e-05
D = 64
NF = 3072
NC = 1024
NB = 12
HALO = 128
BLK = 512
bf16 = jnp.bfloat16
f32 = jnp.float32
i16 = jnp.int16
FACTOR = 1.0 / math.sqrt(393216)


def mm(a, b):
    return jnp.dot(a, b, preferred_element_type=f32)


def mm_last(a, b):
    return lax.dot_general(a, b, (((1,), (1,)), ((), ())), preferred_element_type=f32)


def rows_of(index):
    return jnp.broadcast_to(index, (16, index.shape[1])).astype(i16)


def selector(rows, tile):
    width = rows.shape[1]
    iota = lax.broadcasted_iota(jnp.int32, (256, 128), 0).astype(i16)
    iota = jnp.concatenate([iota] * (width // 128), axis=1)
    key = jnp.concatenate([rows - i16(256 * tile)] * 16, axis=0)
    return jnp.where(iota == key, bf16(1), bf16(0))


def columns_of(index):
    width = index.shape[1]
    sub = lax.broadcasted_iota(jnp.int32, (8, width), 0)
    low, high = index & 255, index >> 8
    parts = jnp.where(sub == 0, low, jnp.where(sub == 1, high, 0)).astype(f32)
    sub = lax.broadcasted_iota(jnp.int32, (8, 128), 0)
    scale = jnp.where(sub == 0, 1.0, jnp.where(sub == 1, 256.0, 0.0))
    out = lax.dot_general(parts, scale, (((0,), (0,)), ((), ())), preferred_element_type=f32)
    return out.astype(jnp.int32).astype(i16)


def selector_t(column, tile):
    lane = lax.broadcasted_iota(jnp.int32, (16, 128), 1).astype(i16)
    halves = []
    for half in range(2):
        key = jnp.concatenate([lane + i16(256 * tile + 128 * half)] * (column.shape[0] // 16), axis=0)
        halves.append(jnp.where(column == key, bf16(1), bf16(0)))
    return jnp.concatenate(halves, axis=1)


def staged(stages, count):
    for step in range(count + len(stages) - 1):
        for depth, stage in enumerate(stages):
            if 0 <= step - depth < count:
                stage(step - depth)


def block_at(i):
    return slice(i * BLK, i * BLK + BLK)


def column_of(row):
    sub = lax.broadcasted_iota(jnp.int32, (D, D), 0)
    lane = lax.broadcasted_iota(jnp.int32, (D, D), 1)
    col = jnp.sum(jnp.where(sub == lane, row, 0.0), axis=1, keepdims=True)
    return jnp.broadcast_to(col, (D, 128))


def wide(col, width):
    return jnp.concatenate([col] * (width // 128), axis=1)


def fold_lanes(values):
    total = values[:, 0:128]
    for begin in range(128, values.shape[1], 128):
        total = total + values[:, begin : begin + 128]
    return total


def mean_rows(values):
    return jnp.sum(values, axis=0, keepdims=True) * (1.0 / D)


def logistic(values):
    return 0.5 * jnp.tanh(0.5 * values) + 0.5


def standardize(values):
    centered = values - mean_rows(values)
    spread = lax.rsqrt(mean_rows(centered * centered) + EPSILON)
    return centered * spread, spread


def normalize_back(upstream, scaled, spread, gain):
    weighted = upstream * gain
    return spread * (weighted - mean_rows(weighted) - scaled * mean_rows(weighted * scaled))


def make_kernel(comm):
    def kernel(
        *refs
    ):
        given, refs = refs[:16], refs[16:]
        (dstate, dedges, packed), refs = refs[:3], refs[3:]
        held, refs = refs[:16], refs[16:]
        (
            stk, slope, scl, ups, spr, msg, ehd, col_s, col_r, col_p,
            sendb, ghost, gsend, gback, nin, nh2, nbr, own, nslope, acc, gac, gt,
            vec, sums, grads, eacc, shared, rs_buf, ex_buf, ag_buf, w1, w2t, nw1, nw2t,
            sem_fs, sem_fr, sem_bs, sem_br, sem_rs, sem_rr, sem_es, sem_er, sem_as, sem_ar,
            sem_in,
        ) = refs
        ns, es, snd, rcv, six, nct, ect, w1t, b1, w2, eg, esh, nw1t, nb1, nw2, ng = held
        loads = [
            pltpu.make_async_copy(given[k], held[k], sem_in.at[k]) for k in range(16)
        ]
        for k in (4, 0, 2, 3, 1, 7, 8, 9, 10, 11, 12, 13, 14, 15, 5, 6):
            loads[k].start()
        if comm:
            z = lax.axis_index("z")
            y = lax.axis_index("y")
            core = lax.axis_index("core")
            s = lax.axis_index("sub")
            d = z * 8 + y * 2 + core
            a = z * 2 + core
            b = y * 4 + s

            def row_peer(step, t):
                dd = lax.rem(d + (step + 32), 32)
                return lax.div(dd, 8), lax.rem(lax.div(dd, 2), 4), lax.rem(dd, 2), t

            far = (0, 1, 2, 1)
            a_steps = sorted(range(1, 8), key=lambda j: -2 * far[j // 2] - j % 2)
            b_steps = sorted(range(1, 16), key=lambda j: -far[j // 4] - far[j % 4])

            def a_peer(j):
                step = a_steps[j - 1]
                far_z = lax.rem(z + step // 2, 4)
                far_core = lax.rem(core + step % 2, 2)
                return far_z * 2 + far_core, (far_z, y, far_core, s)

            def b_peer(j):
                step = b_steps[j - 1]
                far_y = lax.rem(y + step // 4, 4)
                far_s = lax.rem(s + step % 4, 4)
                return far_y * 4 + far_s, (z, far_y, core, far_s)

            halo_pairs = [(o, r) for o in range(3) for r in range(4) if not (o == 1 and r == 0)]
            barrier = pltpu.get_barrier_semaphore()
            peers = [row_peer(o - 1, lax.rem(s + r, 4)) for o, r in halo_pairs]
            peers += [a_peer(j)[1] for j in range(1, 8)] + [b_peer(j)[1] for j in range(1, 16)]
            for peer in peers:
                pl.semaphore_signal(barrier, inc=1, device_id=peer, device_id_type=MESH)
        else:
            s = 0

        def waits(copies):
            for condition, copy in copies:
                if condition is None:
                    copy.wait_send()
                else:
                    pl.when(condition)(copy.wait_send)

        def send_block(k, source, target, sems, turn):
            o, t = k // 4, k % 4
            copy = pltpu.make_async_remote_copy(
                src_ref=source.at[k],
                dst_ref=target.at[o * 4 + s],
                send_sem=sems[0].at[k],
                recv_sem=sems[1].at[o * 4 + s],
                device_id=row_peer(turn * (o - 1), t),
                device_id_type=MESH,
            )
            condition = s != t if o == 1 else None
            if condition is None:
                copy.start()
            else:
                pl.when(condition)(copy.start)
            return condition, copy

        def receive_blocks(source, target, sems):
            for o, r in halo_pairs:
                slot = o * 4 + lax.rem(s + r, 4)
                pltpu.make_async_remote_copy(
                    src_ref=source.at[slot],
                    dst_ref=target.at[slot],
                    send_sem=sems[0].at[0],
                    recv_sem=sems[1].at[slot],
                    device_id=row_peer(o - 1, lax.rem(s + r, 4)),
                    device_id_type=MESH,
                ).wait_recv()

        loads[4].wait()
        loads[0].wait()
        forward = []
        for place, pair in enumerate((0, 1, 4, 5, 2, 3)):
            rows = rows_of(six[:, 256 * pair : 256 * pair + 256])
            picked = jnp.zeros((D, 256), f32)
            for tile in range(4):
                picked = picked + mm(ns[:, 256 * tile : 256 * tile + 256], selector(rows, tile))
            picked = picked.astype(bf16)
            sendb[2 * pair] = picked[:, :HALO]
            sendb[2 * pair + 1] = picked[:, HALO:]
            if comm:
                if place == 0:
                    pl.semaphore_wait(barrier, len(peers))
                for k in (2 * pair, 2 * pair + 1):
                    forward.append(send_block(k, sendb, ghost, (sem_fs, sem_fr), 1))

        ghost[4 + s] = jnp.zeros((D, HALO), bf16)
        gback[4 + s] = jnp.zeros((D, HALO), bf16)
        for k in (2, 3, 1, 7, 8, 9, 10, 11, 12, 13, 14, 15):
            loads[k].wait()
        vec[0] = column_of(b1[...])
        vec[1] = column_of(eg[...])
        vec[2] = column_of(esh[...])
        vec[3] = column_of(nb1[...])
        vec[4] = column_of(ng[...])
        w1[...] = w1t[...].astype(f32).T.astype(bf16)
        w2t[...] = w2[...].astype(f32).T.astype(bf16)
        nw1[...] = nw1t[...].astype(f32).T.astype(bf16)
        nw2t[...] = nw2[...].astype(f32).T.astype(bf16)
        sums[...] = jnp.zeros_like(sums)
        stk[128:192, :] = es[...]
        nin[0:64, :] = ns[...]

        def gather_own(i):
            at = block_at(i)
            for index, begin in ((snd, 0), (rcv, 64)):
                rows = rows_of(index[:, at])
                total = jnp.zeros((D, BLK), f32)
                for tile in range(4):
                    total = total + mm(ns[:, 256 * tile : 256 * tile + 256], selector(rows, tile))
                stk[begin : begin + 64, at] = total.astype(bf16)
            col_r[at, :] = columns_of(rcv[:, at])
            col_s[at, :] = columns_of(snd[:, at])

        staged([gather_own], NF // BLK)
        for pair in range(NB // 2):
            at = slice(256 * pair, 256 * pair + 256)
            col_p[at, :] = columns_of(six[:, at])

        if comm:
            receive_blocks(sendb, ghost, (sem_fs, sem_fr))

        def gather_ghosts(i):
            at = block_at(i)
            rows = rows_of(snd[:, at])
            total = stk[0:64, at].astype(f32)
            for pair in range(NB // 2):
                table = jnp.concatenate([ghost[2 * pair], ghost[2 * pair + 1]], axis=1)
                total = total + mm(table, selector(rows, 4 + pair))
            stk[0:64, at] = total.astype(bf16)

        def forward_faces(i):
            at = block_at(i)
            linear = mm(w1t[...], stk[0:192, at]) + wide(vec[0], BLK)
            gate = logistic(linear)
            activated = linear * gate
            active = activated.astype(bf16)
            stk[192:256, at] = active
            slope[:, at] = gate + activated * (1.0 - gate)

        def forward_norms(i):
            at = block_at(i)
            scaled, spread = standardize(mm(w2t[...], stk[192:256, at]))
            scl[:, at] = scaled
            spr[:, at] = spread
            msg[:, at] = (scaled * wide(vec[1], BLK) + wide(vec[2], BLK)).astype(bf16)

        def scatter(i, part, column, total, tiles, first):
            for tile in tiles:
                where = slice(256 * (tile - tiles[0]), 256 * (tile - tiles[0]) + 256)
                added = mm(part, selector_t(column, tile))
                total[:, where] = added if first else total[:, where] + added

        def sum_messages(i):
            at = block_at(i)
            scatter(i, msg[:, at], col_r[at, :], acc, range(4), i == 0)

        staged([gather_ghosts, forward_faces, forward_norms, sum_messages], NF // BLK)

        loads[5].wait()
        loads[6].wait()
        def cells(i):
            at = block_at(i)
            nin[64:128, at] = acc[:, at].astype(bf16)
            linear = mm(nw1t[...], nin[0:128, at]) + wide(vec[3], BLK)
            gate = logistic(linear)
            activated = linear * gate
            active = activated.astype(bf16)
            nin[128:192, at] = active
            nslope[:, at] = gate + activated * (1.0 - gate)

        def cell_norms(i):
            at = block_at(i)
            scaled, spread = standardize(mm(nw2t[...], nin[128:192, at]))
            upstream = nct[:, at].astype(f32)
            sums[4] += fold_lanes(upstream * scaled)
            sums[5] += fold_lanes(upstream)
            delta = normalize_back(upstream, scaled, spread, wide(vec[4], BLK)).astype(bf16)
            nh2[0:64, at] = delta

        def cell_hidden(i):
            at = block_at(i)
            upstream = nct[:, at].astype(f32)
            hidden = mm(nw2[...], nh2[0:64, at]) * nslope[:, at]
            sums[3] += fold_lanes(hidden)
            hidden = hidden.astype(bf16)
            nh2[64:128, at] = hidden
            back = mm(nw1[...], hidden)
            own[:, at] = back[0:64] + upstream
            nbr[:, at] = back[64:128].astype(bf16)

        staged([cells, cell_norms, cell_hidden], NC // BLK)

        def gather_back(i):
            at = block_at(i)
            rows = rows_of(rcv[:, at])
            upstream = ect[:, at].astype(f32)
            for tile in range(4):
                upstream = upstream + mm(
                    nbr[:, 256 * tile : 256 * tile + 256], selector(rows, tile)
                )
            ups[:, at] = upstream

        def backward_faces(i):
            at = block_at(i)
            upstream = ups[:, at]
            scaled = scl[:, at]
            sums[1] += fold_lanes(upstream * scaled)
            sums[2] += fold_lanes(upstream)
            delta = normalize_back(upstream, scaled, spr[:, at], wide(vec[1], BLK)).astype(bf16)
            ehd[64:128, at] = delta

        def backward_hidden(i):
            at = block_at(i)
            hidden = mm(w2[...], ehd[64:128, at]) * slope[:, at]
            sums[0] += fold_lanes(hidden)
            ehd[0:64, at] = hidden.astype(bf16)

        def weigh_faces(i):
            at = block_at(i)
            part = mm_last(stk[:, at], ehd[:, at])
            eacc[...] = part if i == 0 else eacc[...] + part

        staged([gather_back, backward_faces, backward_hidden, weigh_faces], NF // BLK)

        edge_part = eacc[...]
        node_part = mm_last(nin[...], nh2[...])
        lane64 = lax.broadcasted_iota(jnp.int32, (64, 128), 1)
        vectors = jnp.zeros((64, 128), f32)
        for number in range(6):
            vectors = jnp.where(
                lane64 == 64 + number, jnp.sum(sums[number], axis=1, keepdims=True), vectors
            )
        high = vectors.astype(bf16).astype(f32)
        vectors = high + pltpu.roll(vectors - high, 6, 1)
        grads[0:64] = jnp.where(lane64 < 64, edge_part[0:64], node_part[0:64])
        grads[64:128] = jnp.where(lane64 < 64, edge_part[64:128], node_part[64:128])
        grads[128:192] = jnp.where(lane64 < 64, edge_part[128:192], vectors)
        grads[192:256] = jnp.where(lane64 < 64, node_part[128:192], edge_part[192:256])

        first = []
        if comm:
            shared[...] = grads[...].astype(bf16)
            for j in range(1, 8):
                other, peer = a_peer(j)
                first.append(
                    pltpu.make_async_remote_copy(
                        src_ref=shared.at[pl.ds(pl.multiple_of(other * 32, 32), 32), :],
                        dst_ref=rs_buf.at[a],
                        send_sem=sem_rs.at[j],
                        recv_sem=sem_rr.at[a],
                        device_id=peer,
                        device_id_type=MESH,
                    )
                )
            for copy in first:
                copy.start()

        def sum_ghosts(i):
            at = block_at(i)
            scatter(i, ehd[0:64, at], col_s[at, :], gac, range(4, 10), i == 0)

        staged([sum_ghosts], NF // BLK)
        def split_vectors(total):
            lane = lax.broadcasted_iota(jnp.int32, (32, 128), 1)
            whole = total + pltpu.roll(total, 122, 1)
            high = whole.astype(bf16).astype(f32)
            parts = jnp.where(lane < 70, high, pltpu.roll(whole - high, 6, 1))
            return jnp.where(((a == 4) | (a == 5)) & (lane >= 64) & (lane < 76), parts, total)

        second = []
        if comm:
            total = grads[pl.ds(pl.multiple_of(a * 32, 32), 32), :]
            for j in range(1, 8):
                other, peer = a_peer(j)
                pltpu.make_async_remote_copy(
                    src_ref=rs_buf.at[other],
                    dst_ref=rs_buf.at[other],
                    send_sem=sem_rs.at[j],
                    recv_sem=sem_rr.at[other],
                    device_id=peer,
                    device_id_type=MESH,
                ).wait_recv()
                total = total + rs_buf[other].astype(f32)
            ex_buf[b] = split_vectors(total).astype(bf16)
            for j in range(1, 16):
                other, peer = b_peer(j)
                second.append(
                    pltpu.make_async_remote_copy(
                        src_ref=ex_buf.at[b],
                        dst_ref=ex_buf.at[b],
                        send_sem=sem_es.at[j],
                        recv_sem=sem_er.at[b],
                        device_id=peer,
                        device_id_type=MESH,
                    )
                )
            for copy in second:
                copy.start()

        backward = []
        for pair in (0, 1, 4, 5, 2, 3):
            block = mm(w1[0:64, :], gac[:, 256 * pair : 256 * pair + 256].astype(bf16)).astype(bf16)
            gsend[2 * pair] = block[:, :HALO]
            gsend[2 * pair + 1] = block[:, HALO:]
            if comm:
                for k in (2 * pair, 2 * pair + 1):
                    backward.append(send_block(k, gsend, gback, (sem_bs, sem_br), -1))

        def sum_senders(i):
            at = block_at(i)
            scatter(i, ehd[0:64, at], col_s[at, :], acc, range(4), i == 0)

        staged([sum_senders], NF // BLK)

        def sum_receivers(i):
            at = block_at(i)
            scatter(i, ehd[0:64, at], col_r[at, :], gt, range(4), i == 0)

        staged([sum_receivers], NF // BLK)
        own[...] += mm(w1[0:64, :], acc[...].astype(bf16)) + mm(w1[64:128, :], gt[...].astype(bf16))

        for i in range(NF // BLK):
            at = block_at(i)
            dedges[:, at] = (ect[:, at].astype(f32) + mm(w1[128:192, :], ehd[0:64, at])).astype(bf16)

        third = []
        if comm:
            for j in range(1, 16):
                other, peer = b_peer(j)
                pltpu.make_async_remote_copy(
                    src_ref=ex_buf.at[other],
                    dst_ref=ex_buf.at[other],
                    send_sem=sem_es.at[j],
                    recv_sem=sem_er.at[other],
                    device_id=peer,
                    device_id_type=MESH,
                ).wait_recv()
            total = ex_buf[0].astype(f32)
            for j in range(1, 16):
                total = total + ex_buf[j].astype(f32)
            ag_buf[a] = split_vectors(total).astype(bf16)
            for j in range(1, 8):
                other, peer = a_peer(j)
                third.append(
                    pltpu.make_async_remote_copy(
                        src_ref=ag_buf.at[a],
                        dst_ref=ag_buf.at[a],
                        send_sem=sem_as.at[j],
                        recv_sem=sem_ar.at[a],
                        device_id=peer,
                        device_id_type=MESH,
                    )
                )
            for copy in third:
                copy.start()

        if comm:
            receive_blocks(gsend, gback, (sem_bs, sem_br))

        returned = jnp.concatenate([gback[k] for k in range(NB)], axis=1)
        for tile in range(4):
            where = slice(256 * tile, 256 * tile + 256)
            total = own[:, where]
            for pair in range(NB // 2):
                at = slice(256 * pair, 256 * pair + 256)
                total = total + mm(returned[:, at], selector_t(col_p[at, :], tile))
            dstate[:, where] = total.astype(bf16)

        if comm:
            for j in range(1, 8):
                other, peer = a_peer(j)
                pltpu.make_async_remote_copy(
                    src_ref=ag_buf.at[other],
                    dst_ref=ag_buf.at[other],
                    send_sem=sem_as.at[j],
                    recv_sem=sem_ar.at[other],
                    device_id=peer,
                    device_id_type=MESH,
                ).wait_recv()
            for j in range(8):
                packed[32 * j : 32 * j + 32] = ag_buf[j].astype(f32)
        else:
            packed[...] = grads[...]
        waits(forward + backward)
        for copy in first + second + third:
            copy.wait_send()

    return kernel


def finish(
    dstate, dedges, packed, out_state, out_edges, *refs
):
    results, refs = refs[:10], refs[10:]
    staged, sems = refs[:10], refs[10]
    o_w1, o_b1, o_w2, o_eg, o_es, o_nw1, o_nb1, o_nw2, o_ng, o_ns = staged
    stores = [
        pltpu.make_async_copy(dedges, out_edges, sems.at[10]),
        pltpu.make_async_copy(dstate, out_state, sems.at[11]),
    ]
    for copy in stores:
        copy.start()
    whole = packed[...] * FACTOR
    turned = jnp.concatenate([whole[0:128].T, whole[128:256].T], axis=1)
    o_w1[...] = turned[0:64, 0:192]
    o_nw1[...] = turned[64:128, 0:128]
    o_nw2[...] = whole[192:256, 0:64]
    o_w2[...] = pltpu.roll(whole[192:256], 64, 1)[:, 0:64]
    rows = turned[64:128, 128:192]
    for k, ref in enumerate((o_b1, o_eg, o_es, o_nb1, o_ng, o_ns)):
        ref[...] = rows[k : k + 1, :] + rows[k + 6 : k + 7, :]
    for k in range(10):
        copy = pltpu.make_async_copy(staged[k], results[k], sems.at[k])
        copy.start()
        stores.append(copy)
    for copy in stores:
        copy.wait()


def call(comm, *args):
    shapes = [
        ((D, NC), bf16),
        ((D, NF), bf16),
        ((64, 192), f32),
        ((1, 64), f32),
        ((64, 64), f32),
        ((1, 64), f32),
        ((1, 64), f32),
        ((64, 128), f32),
        ((1, 64), f32),
        ((64, 64), f32),
        ((1, 64), f32),
        ((1, 64), f32),
    ]
    dma = pltpu.SemaphoreType.DMA
    scratch = [pltpu.VMEM(arg.shape, arg.dtype) for arg in args]
    scratch += [
        pltpu.VMEM((256, NF), bf16),
        pltpu.VMEM((D, NF), f32),
        pltpu.VMEM((D, NF), f32),
        pltpu.VMEM((D, NF), f32),
        pltpu.VMEM((1, NF), f32),
        pltpu.VMEM((D, NF), bf16),
        pltpu.VMEM((128, NF), bf16),
        pltpu.VMEM((NF, 128), i16),
        pltpu.VMEM((NF, 128), i16),
        pltpu.VMEM((NB * HALO, 128), i16),
        pltpu.VMEM((NB, D, HALO), bf16),
        pltpu.VMEM((NB, D, HALO), bf16),
        pltpu.VMEM((NB, D, HALO), bf16),
        pltpu.VMEM((NB, D, HALO), bf16),
        pltpu.VMEM((192, NC), bf16),
        pltpu.VMEM((128, NC), bf16),
        pltpu.VMEM((D, NC), bf16),
        pltpu.VMEM((D, NC), f32),
        pltpu.VMEM((D, NC), f32),
        pltpu.VMEM((D, NC), f32),
        pltpu.VMEM((D, NB * HALO), f32),
        pltpu.VMEM((D, NC), f32),
        pltpu.VMEM((5, D, 128), f32),
        pltpu.VMEM((6, D, 128), f32),
        pltpu.VMEM((256, 128), f32),
        pltpu.VMEM((256, 128), f32),
        pltpu.VMEM((256, 128), bf16),
        pltpu.VMEM((8, 32, 128), bf16),
        pltpu.VMEM((16, 32, 128), bf16),
        pltpu.VMEM((8, 32, 128), bf16),
        pltpu.VMEM((192, 64), bf16),
        pltpu.VMEM((64, 64), bf16),
        pltpu.VMEM((128, 64), bf16),
        pltpu.VMEM((64, 64), bf16),
        dma((12,)), dma((12,)), dma((12,)), dma((12,)),
        dma((8,)), dma((8,)), dma((16,)), dma((16,)), dma((8,)), dma((8,)),
        dma((16,)),
    ]
    anywhere = pl.BlockSpec(memory_space=pltpu.HBM)
    params = dict(vmem_limit_bytes=36 * 1024 * 1024)
    if comm:
        params.update(collective_id=0, has_side_effects=True)
    vmem = pl.BlockSpec(memory_space=pltpu.VMEM)
    middle = pl.pallas_call(
        make_kernel(comm),
        out_shape=[
            jax.ShapeDtypeStruct(shape, kind) for shape, kind in shapes[:2] + [((256, 128), f32)]
        ],
        in_specs=[anywhere] * 16,
        out_specs=[vmem] * 3,
        scratch_shapes=scratch,
        compiler_params=pltpu.CompilerParams(**params),
        name="layer",
    )(*[pltpu.with_memory_space_constraint(arg, pltpu.HBM) for arg in args])
    return pl.pallas_call(
        finish,
        out_shape=[jax.ShapeDtypeStruct(shape, kind) for shape, kind in shapes],
        in_specs=[vmem] * 3,
        out_specs=[anywhere] * 12,
        scratch_shapes=[pltpu.VMEM(shape, kind) for shape, kind in shapes[2:]] + [dma((12,))],
        compiler_params=pltpu.CompilerParams(vmem_limit_bytes=8 * 1024 * 1024),
        name="finish",
    )(*middle)


def on_device(comm, node_state, edge_state, senders, receivers, send_index, node_cotangent, edge_cotangent,
              edge_first, edge_bias, edge_second, edge_gain, edge_shift, node_first, node_bias, node_second, node_gain):
    line = lambda v: v.reshape(1, -1)
    outs = call(
        comm, node_state, edge_state, line(senders), line(receivers), line(send_index),
        node_cotangent, edge_cotangent, edge_first.T, line(edge_bias), edge_second, line(edge_gain),
        line(edge_shift), node_first.T, line(node_bias), node_second, line(node_gain),
    )
    outs = [v.reshape(-1) if v.shape[0] == 1 else v for v in outs]
    outs[2] = outs[2].T
    outs[7] = outs[7].T
    return tuple(outs)


def solution(mesh):
    split = Mesh(mesh.devices.reshape(4, 4, 2, 4), AXES)
    every = P(None, AXES)
    in_specs = (every, every, P(AXES), P(AXES), P(AXES, None, None), every, every) + (P(),) * 9
    out_specs = (every, every) + (P(),) * 10
    return jax.shard_map(
        lambda *args: on_device(True, *args), mesh=split, in_specs=in_specs, out_specs=out_specs,
        check_vma=False,
    )
```
